512 devices in a mesh: dp: 16 (over x, z_hi, core), shard: 32 (over z_lo, y).
Axes of the slice: x: 4, y: 4, z: 16 (z_hi: 2, z_lo: 8; z = z_hi * 8 + z_lo), core: 2. Of those that a mesh axis runs over, the one named last changes fastest.
Arguments:
- tokens: bfloat16 [1024, 6144], P('dp', 'shard'), may hold values from -6 to 6
- cotangent: bfloat16 [1024, 6144], P('dp', 'shard'), may hold values from -12 to 12
- gate_proj: bfloat16 [2, 6144, 16384], P(None, 'dp', 'shard'), may hold values from -0.078125 to 0.078125
- up_proj: bfloat16 [2, 6144, 16384], P(None, 'dp', 'shard'), may hold values from -0.078125 to 0.078125
- down_proj: bfloat16 [2, 16384, 6144], P(None, 'shard', 'dp'), may hold values from -0.046875 to 0.046875
- slot_tokens: int32 [2, 256], P(None, 'dp'), may hold values from 0 to 63, as said below
- gate_weights: float32 [2, 256], P(None, 'dp'), may hold values from 0.1 to 1
- live_counts: int32 [2, 16], P(None, 'dp'), may hold values from 1 to 16, as said below
Outputs:
- grad_tokens: bfloat16 [1024, 6144], P('dp', 'shard')
- grad_gate_proj: bfloat16 [2, 6144, 16384], P(None, 'dp', 'shard')
- grad_up_proj: bfloat16 [2, 6144, 16384], P(None, 'dp', 'shard')
- grad_down_proj: bfloat16 [2, 16384, 6144], P(None, 'shard', 'dp')
The draws below stay inside these ranges and needn't reach their ends.
Inputs may be any that keep to these rules, and one draw needn't show every extreme that they name: `slot_tokens`: for each expert and each index of dp, the 16 slots name 16 different tokens of that index. `live_counts`: the live slots of an expert at an index of dp are its first ones; 16 is reached at some index of every expert.
All inputs are finite; a program needn't handle non-finite values.
Results may differ from the reference program's by a relative error of at most 0.03.
Values may be sent and summed in bfloat16 or wider, within the bound.
No kernel may reach another device: no remote copies, remote signals or barrier semaphores. Data moves between devices by JAX's collectives and lax.ppermute only.
A program may use at most 64 MiB of HBM per device.

```python
import jax
import jax.numpy as jnp
from jax import lax

D = 6144
FF = 16384
EXPERTS = 2
ROWS = 16
TOK_DEV = 64
TOKENS = 1024
ROUTED = 256
N_DP = 16
N_SHARD = 32


def draw_slot_tokens(key, part):
    shape = (EXPERTS, N_DP, TOK_DEV)
    scores = jax.random.randint(key, shape, 0, 1 << 20)
    scores = scores * TOK_DEV + lax.broadcasted_iota(jnp.int32, shape, 2)
    chosen = jnp.argsort(scores, axis=2, stable=True)[:, :, :ROWS]
    return chosen.reshape(EXPERTS, N_DP * ROWS).astype(jnp.int32)


def draw_live_counts(key, part):
    lowest = max(ROWS // 3, 1)
    position = lax.broadcasted_iota(jnp.int32, (EXPERTS, N_DP), 1)
    rising = lowest + position * (ROWS - lowest) // max(N_DP - 1, 1)
    jitter = jax.random.randint(key, (EXPERTS, N_DP), -2, 3)
    drawn = jnp.clip(rising + jitter, 1, ROWS)
    return jnp.where(position == N_DP - 1, ROWS, drawn).astype(jnp.int32)


def shard_levels(key, shape, shards, least, top_value):
    gain, own = 1.0, jax.random.fold_in(key, 6)
    for dim, shards_of in shards:
        heights = jnp.exp(jax.random.uniform(jax.random.fold_in(own, dim), (shards_of,), jnp.float32, least / len(shards), top_value / len(shards)))
        gain = gain * jnp.repeat(heights, shape[dim] // shards_of).reshape([-1 if axis == dim else 1 for axis in range(len(shape))])
    return gain


def centred(key, dims, spread, reach, shards=(), kind=jnp.bfloat16):
    values = jax.random.normal(key, dims, jnp.float32) * spread
    if len(shards) > 0:
        values = shard_levels(key, dims, shards, -0.22, 0.18) * values
    return jnp.clip(values, min=-reach, max=reach).astype(kind)


def setup_inputs(seed: int = 0) -> dict:
    streams_of = jax.random.split(jax.random.key(seed), 9)
    tokens = centred(streams_of[0], (TOKENS, D), 1.0, 6.0, ((0, 16), (1, 32)))
    cotangent = centred(streams_of[1], (TOKENS, D), 2.0, 12.0, ((0, 16), (1, 32)))
    gate_proj = centred(streams_of[2], (EXPERTS, D, FF), D ** -0.5, 0.078125, ((1, 16), (2, 32)))
    up_proj = centred(streams_of[3], (EXPERTS, D, FF), D ** -0.5, 0.078125, ((1, 16), (2, 32)))
    down_proj = centred(streams_of[4], (EXPERTS, FF, D), FF ** -0.5, 0.046875, ((1, 32), (2, 16)))
    slot_tokens = draw_slot_tokens(jax.random.fold_in(streams_of[8], 71), 0)
    gate_weights = jnp.clip(0.1 + 0.9 * jax.random.uniform(streams_of[6], (EXPERTS, ROUTED), jnp.float32) ** shard_levels(streams_of[6], (EXPERTS, ROUTED), ((1, 16),), -0.2, 0.2), 0.1, 1.0)
    live_counts = draw_live_counts(jax.random.fold_in(streams_of[8], 71), 0)
    return {"tokens": tokens, "cotangent": cotangent, "gate_proj": gate_proj, "up_proj": up_proj, "down_proj": down_proj, "slot_tokens": slot_tokens, "gate_weights": gate_weights, "live_counts": live_counts}


def rounded(term):
    return lax.optimization_barrier(term.astype(jnp.bfloat16)).astype(jnp.float32)


def slope_terms(gate_sum, up_sum, cot_hidden):
    sigmoid_part = jax.nn.sigmoid(gate_sum)
    grad_gate = (cot_hidden * up_sum * sigmoid_part * (1.0 + gate_sum * (1.0 - sigmoid_part))).astype(jnp.bfloat16)
    grad_up = (cot_hidden * gate_sum * sigmoid_part).astype(jnp.bfloat16)
    return grad_gate, grad_up


def reference(tokens, cotangent, gate_proj, up_proj, down_proj, slot_tokens, gate_weights, live_counts):
    routed = N_DP * ROWS
    position = lax.broadcasted_iota(jnp.int32, (EXPERTS, routed), 1)
    owner = (position // ROWS).astype(jnp.int32)
    places = (slot_tokens + owner * TOK_DEV).astype(jnp.int32)
    alive_mask = ((position % ROWS) < jnp.take_along_axis(live_counts, owner, axis=1)).astype(jnp.float32)
    picked = tokens[places]
    weighted = (cotangent[places].astype(jnp.float32) * (gate_weights * alive_mask)[:, :, None]).astype(jnp.bfloat16)
    totals = jnp.sum(live_counts, axis=1).astype(jnp.float32)
    picked_wide = picked.astype(jnp.float32)
    weighted_wide = weighted.astype(jnp.float32)
    span = D // N_DP
    blocks_dp = jnp.arange(N_DP, dtype=jnp.int32)

    def input_block(carry, block):
        start = block * span
        rows_part = lax.dynamic_slice_in_dim(picked_wide, start, span, 2)
        gate_rows = lax.dynamic_slice_in_dim(gate_proj, start, span, 1).astype(jnp.float32)
        up_rows = lax.dynamic_slice_in_dim(up_proj, start, span, 1).astype(jnp.float32)
        gate_part = jnp.einsum('erd,edf->erf', rows_part, gate_rows)
        up_part = jnp.einsum('erd,edf->erf', rows_part, up_rows)
        return (carry[0] + rounded(gate_part), carry[1] + rounded(up_part)), None

    zeros_hidden = jnp.zeros((EXPERTS, routed, FF), jnp.float32)
    (gate_sum, up_sum), _ = lax.scan(input_block, (zeros_hidden, zeros_hidden), blocks_dp)
    hidden = (jax.nn.silu(gate_sum) * up_sum).astype(jnp.bfloat16)

    def cot_block(carry, block):
        start = block * span
        cot_part = lax.dynamic_slice_in_dim(weighted_wide, start, span, 2)
        down_cols = lax.dynamic_slice_in_dim(down_proj, start, span, 2).astype(jnp.float32)
        return carry + rounded(jnp.einsum('erd,efd->erf', cot_part, down_cols)), None

    cot_hidden, _ = lax.scan(cot_block, zeros_hidden, blocks_dp)
    grad_gate, grad_up = slope_terms(gate_sum, up_sum, cot_hidden)

    def expert_grads(pieces):
        rows_in, cot_in, hidden_in, gate_in, up_in, total = pieces
        gate_grad = (jnp.dot(rows_in.T, gate_in, preferred_element_type=jnp.float32) / total).astype(jnp.bfloat16)
        up_grad = (jnp.dot(rows_in.T, up_in, preferred_element_type=jnp.float32) / total).astype(jnp.bfloat16)
        down_grad = (jnp.dot(hidden_in.T, cot_in, preferred_element_type=jnp.float32) / total).astype(jnp.bfloat16)
        return gate_grad, up_grad, down_grad

    grad_gate_proj, grad_up_proj, grad_down_proj = lax.map(
        expert_grads, (picked, weighted, hidden, grad_gate, grad_up, totals))

    width = FF // N_SHARD
    gate_wide = grad_gate.astype(jnp.float32)
    up_wide = grad_up.astype(jnp.float32)

    def back_block(carry, block):
        start = block * width
        gate_cols = lax.dynamic_slice_in_dim(gate_wide, start, width, 2)
        up_cols = lax.dynamic_slice_in_dim(up_wide, start, width, 2)
        gate_mat = lax.dynamic_slice_in_dim(gate_proj, start, width, 2).astype(jnp.float32)
        up_mat = lax.dynamic_slice_in_dim(up_proj, start, width, 2).astype(jnp.float32)
        term = jnp.einsum('erf,edf->erd', gate_cols, gate_mat) + jnp.einsum('erf,edf->erd', up_cols, up_mat)
        return carry + rounded(term), None

    grad_rows, _ = lax.scan(back_block, jnp.zeros((EXPERTS, routed, D), jnp.float32),
                            jnp.arange(N_SHARD, dtype=jnp.int32))
    grad_tokens = jnp.zeros((TOKENS, D), jnp.float32).at[places.reshape(-1)].add(
        grad_rows.reshape(EXPERTS * routed, D)).astype(jnp.bfloat16)
    return grad_tokens, grad_gate_proj, grad_up_proj, grad_down_proj
```

```python
import jax
import jax.numpy as jnp
from jax import lax
from jax.experimental import pallas as pl
from jax.experimental.pallas import tpu as pltpu
from jax.sharding import Mesh, PartitionSpec as P

X, ZH, C, ZL, Y = 4, 2, 2, 8, 4
DP = ("x", "zh", "c")
SHARD = ("zl", "y")
EVERY = DP + SHARD
N_SHARD = ZL * Y
HALF = 192
WIDE = 256
R = 16
BF16 = jnp.bfloat16
F32 = jnp.float32


def outward():
    return [
        (k * N_SHARD + s, (s // 2) * N_SHARD + 2 * k + s % 2)
        for k in range(X * ZH * C)
        for s in range(N_SHARD)
    ]


def homeward():
    return [(there, here) for here, there in outward()]


def dot(a, b, dims):
    return lax.dot_general(a, b, (dims, ((), ())), preferred_element_type=F32)


def as_column(row):
    n = row.shape[1]
    eye = lax.broadcasted_iota(jnp.int32, (n, n), 0) == lax.broadcasted_iota(jnp.int32, (n, n), 1)
    return jnp.sum(jnp.where(eye, jnp.broadcast_to(row, (n, n)), 0), axis=1, keepdims=True)


def pick_kernel(tok_ref, cot_ref, slot_ref, gate_ref, live_ref, out_ref):
    tokens = tok_ref[...]
    cot = cot_ref[...]
    spot = lax.broadcasted_iota(jnp.int32, (R, 64), 1)
    row = lax.broadcasted_iota(jnp.int32, (R, 1), 0)
    lane = lax.broadcasted_iota(jnp.int32, (R, WIDE - HALF), 1)
    for e in range(2):
        one_hot = (as_column(slot_ref[e : e + 1, :]) == spot).astype(BF16)
        count = live_ref[e]
        scale = jnp.where(row < count, as_column(gate_ref[e : e + 1, :]), 0.0)
        picked = dot(one_hot, tokens, ((1,), (0,)))
        weighted = dot(one_hot, cot, ((1,), (0,))) * scale
        first = jnp.logical_and(lane == 0, row == 0)
        note = jnp.where(first, count.astype(F32), 0.0)
        blank = jnp.zeros_like(note)
        out_ref[e * R : (e + 1) * R, :] = jnp.concatenate([picked, note], axis=1).astype(BF16)
        out_ref[(2 + e) * R : (3 + e) * R, :] = jnp.concatenate([weighted, blank], axis=1).astype(
            BF16
        )


def both_halves(got_ref, half, m, e):
    at = (2 * m + e) * R
    parts = [got_ref[2 * half + h, :, at : at + R, :][:, :, :HALF] for h in range(2)]
    parts = [part.reshape(ZH * X * R, HALF) for part in parts]
    return jnp.concatenate(parts, axis=1)


def forward_kernel(core_ref, got_ref, gate_ref, up_ref, down_ref, send_ref, keep_ref):
    core = core_ref[0]
    for half, out_ref in ((1 - core, send_ref), (core, keep_ref)):
        for e in range(2):
            rows = both_halves(got_ref, half, 0, e)
            cot = both_halves(got_ref, half, 1, e)
            parts = (
                dot(rows, gate_ref[e], ((1,), (0,))),
                dot(rows, up_ref[e], ((1,), (0,))),
                dot(cot, down_ref[e], ((1,), (1,))),
            )
            for t, part in enumerate(parts):
                out_ref[:, 2 * t + e] = part.astype(BF16).reshape(X, ZH * R, 512)


def back_kernel(core_ref, mine_ref, other_ref, gate_ref, up_ref, out_ref):
    core = core_ref[0]
    blank = jnp.zeros((ZH * X * R, WIDE - HALF), BF16)
    for half, in_ref in ((1 - core, other_ref), (core, mine_ref)):
        for e in range(2):
            grad_gate = in_ref[:, 2 + e].reshape(ZH * X * R, 512)
            grad_up = in_ref[:, 4 + e].reshape(ZH * X * R, 512)
            term = (
                dot(grad_gate, gate_ref[e], ((1,), (1,))) + dot(grad_up, up_ref[e], ((1,), (1,)))
            ).astype(BF16)
            for h in range(2):
                piece = jnp.concatenate([term[:, h * HALF : (h + 1) * HALF], blank], axis=1)
                out_ref[2 * half + h, :, e * R : (e + 1) * R, :] = piece.reshape(ZH * X, R, WIDE)


def weight_kernel(core_ref, got_ref, mine_ref, other_ref, gate_out, up_out, down_out):
    core = core_ref[0]
    for e in range(2):
        count = sum(
            jnp.sum(got_ref[2 * half, :, e * R : (e + 1) * R, :][:, :, HALF:].astype(F32))
            for half in range(2)
        )
        scale = 1.0 / jnp.full((1, 512), count, F32)
        rows = [both_halves(got_ref, half, 0, e) for half in (core, 1 - core)]
        cot = [both_halves(got_ref, half, 1, e) for half in (core, 1 - core)]
        rows = jnp.concatenate(rows, axis=0)
        cot = jnp.concatenate(cot, axis=0)

        def whole(t):
            return jnp.concatenate(
                [ref[:, 2 * t + e].reshape(ZH * X * R, 512) for ref in (mine_ref, other_ref)], axis=0
            )

        gate_out[e] = (dot(rows, whole(1), ((0,), (0,))) * scale).astype(BF16)
        up_out[e] = (dot(rows, whole(2), ((0,), (0,))) * scale).astype(BF16)
        down_out[e] = (dot(whole(0), cot, ((0,), (0,))) * scale[:, :384]).astype(BF16)


def place_kernel(rows_ref, slot_ref, out_ref):
    spot = lax.broadcasted_iota(jnp.int32, (64, R), 0)
    total = jnp.zeros((64, HALF), F32)
    for e in range(2):
        one_hot = (spot == slot_ref[e : e + 1, :]).astype(BF16)
        total = total + dot(one_hot, rows_ref[e * R : (e + 1) * R, :][:, :HALF], ((1,), (0,)))
    out_ref[...] = total.astype(BF16)


VM = pl.BlockSpec(memory_space=pltpu.VMEM)
SM = pl.BlockSpec(memory_space=pltpu.SMEM)


def local(kernel, specs, outs, name):
    shapes = [jax.ShapeDtypeStruct(o, BF16) for o in outs]
    return pl.pallas_call(
        kernel,
        in_specs=specs,
        out_specs=[VM] * len(outs),
        out_shape=shapes,
        name=name,
    )


def on_device(
    tokens, cotangent, gate_proj, up_proj, down_proj, slot_tokens, gate_weights, live_counts
):
    core = lax.axis_index("c").astype(jnp.int32).reshape(1)
    (message,) = local(pick_kernel, [VM, VM, VM, VM, SM], [(64, WIDE)], "pick")(
        tokens, cotangent, slot_tokens, gate_weights, live_counts.reshape(2)
    )
    message = lax.ppermute(message, EVERY, outward())
    copies = jnp.broadcast_to(message[None], (ZL, 64, WIDE))
    column = lax.all_to_all(copies, "zl", 0, 0, tiled=True)
    got = lax.all_gather(column, "y", axis=0, tiled=False)

    stage = (X, 6, ZH * R, 512)
    send, keep = local(forward_kernel, [SM, VM, VM, VM, VM], [stage, stage], "forward")(
        core, got, gate_proj, up_proj, down_proj
    )
    swap = [(0, 1), (1, 0)]
    heard = lax.ppermute(send, "c", swap)
    paired = (keep.astype(F32) + heard.astype(F32)).astype(BF16)
    over_x = lax.all_to_all(paired, "x", 0, 0, tiled=True)
    over_x = jnp.sum(over_x.astype(F32), axis=0).astype(BF16)
    over_zh = lax.all_gather(over_x, "zh", axis=0, tiled=False)
    sums = jnp.sum(over_zh.astype(F32), axis=0)
    gate_sum, up_sum, cot_hidden = sums[0:2], sums[2:4], sums[4:6]
    sigmoid_part = jax.nn.sigmoid(gate_sum)
    hidden = gate_sum * sigmoid_part * up_sum
    grad_gate = cot_hidden * up_sum * sigmoid_part * (1.0 + gate_sum * (1.0 - sigmoid_part))
    grad_up = cot_hidden * gate_sum * sigmoid_part
    acts = jnp.concatenate([hidden, grad_gate, grad_up], axis=0).astype(BF16)
    mine = lax.all_gather(acts, "x", axis=0, tiled=False)
    other = lax.ppermute(mine, "c", swap)

    (back,) = local(back_kernel, [SM, VM, VM, VM, VM], [(C * 2, X * ZH, 2 * R, WIDE)], "back")(
        core, mine, other, gate_proj, up_proj
    )
    over_y = lax.all_to_all(back, "y", 0, 0, tiled=True)
    over_y = jnp.sum(over_y.astype(F32), axis=0).astype(BF16)
    over_zl = lax.all_to_all(over_y, "zl", 0, 0, tiled=True)
    over_zl = jnp.sum(over_zl.astype(F32), axis=0).astype(BF16)
    home = lax.ppermute(over_zl, EVERY, homeward())
    grad_gate_proj, grad_up_proj, grad_down_proj = local(
        weight_kernel,
        [SM, VM, VM, VM],
        [gate_proj.shape, up_proj.shape, down_proj.shape],
        "weights",
    )(core, got, mine, other)
    (grad_tokens,) = local(place_kernel, [VM, VM], [tokens.shape], "place")(home, slot_tokens)
    return (grad_tokens, grad_gate_proj, grad_up_proj, grad_down_proj)


def solution(mesh):
    fine = Mesh(mesh.devices.reshape(X, ZH, C, ZL, Y), EVERY)
    in_specs = (
        P(DP, SHARD),
        P(DP, SHARD),
        P(None, DP, SHARD),
        P(None, DP, SHARD),
        P(None, SHARD, DP),
        P(None, DP),
        P(None, DP),
        P(None, DP),
    )
    out_specs = (
        P(DP, SHARD),
        P(None, DP, SHARD),
        P(None, DP, SHARD),
        P(None, SHARD, DP),
    )
    return jax.shard_map(
        on_device, mesh=fine, in_specs=in_specs, out_specs=out_specs, check_vma=False
    )
```

```python
import jax
import jax.numpy as jnp
from jax import lax
from jax.experimental import pallas as pl
from jax.experimental.pallas import tpu as pltpu
from jax.sharding import Mesh, PartitionSpec as P

X, ZH, C, ZL, Y = 4, 2, 2, 8, 4
DP = ("x", "zh", "c")
SHARD = ("zl", "y")
EVERY = DP + SHARD
N_SHARD = ZL * Y
HALF = 192
R = 16
PACK = 3 * R
MESSAGE = 2 * PACK + 8
BF16 = jnp.bfloat16
F32 = jnp.float32


def outward():
    return [
        (k * N_SHARD + s, (s // 2) * N_SHARD + 2 * k + s % 2)
        for k in range(X * ZH * C)
        for s in range(N_SHARD)
    ]


def homeward():
    return [(there, here) for here, there in outward()]


def dot(a, b, dims):
    return lax.dot_general(a, b, (dims, ((), ())), preferred_element_type=F32)


def as_column(row):
    n = row.shape[1]
    eye = lax.broadcasted_iota(jnp.int32, (n, n), 0) == lax.broadcasted_iota(jnp.int32, (n, n), 1)
    return jnp.sum(jnp.where(eye, jnp.broadcast_to(row, (n, n)), 0), axis=1, keepdims=True)


def pick_kernel(
    tok_hbm, cot_hbm, slot_hbm, gate_hbm, live_hbm, out_ref, tok, cot, slots, gates, live, sems
):
    moves = [
        pltpu.make_async_copy(source, target, sems.at[i])
        for i, (source, target) in enumerate(
            (
                (slot_hbm, slots),
                (gate_hbm, gates),
                (live_hbm, live),
                (tok_hbm, tok),
                (cot_hbm, cot),
            )
        )
    ]
    for move in moves:
        move.start()
    for move in moves:
        move.wait()
    spot = lax.broadcasted_iota(jnp.int32, (R, 64), 1)
    row = lax.broadcasted_iota(jnp.int32, (R, 1), 0)
    one_hot = [(as_column(slots[e : e + 1, :]) == spot).astype(BF16) for e in range(2)]
    scale = [jnp.where(row < live[e], as_column(gates[e : e + 1, :]), 0.0) for e in range(2)]
    for m, in_ref in enumerate((tok, cot)):
        values = in_ref[...]
        rows = [dot(one_hot[e], values, ((1,), (0,))) for e in range(2)]
        if m == 1:
            rows = [rows[e] * scale[e] for e in range(2)]
        out_ref[m * PACK : (m + 1) * PACK, :] = packed([part.astype(BF16) for part in rows])
    lane = lax.broadcasted_iota(jnp.int32, (8, 128), 1)
    line = lax.broadcasted_iota(jnp.int32, (8, 128), 0)
    note = jnp.where(lane == 0, live[0], 0) + jnp.where(lane == 64, live[1], 0)
    out_ref[2 * PACK :, :] = jnp.where(line == 0, note, 0).astype(F32).astype(BF16)


def packed(rows):
    left = jnp.concatenate([part[:, 128:] for part in rows], axis=1)
    return jnp.concatenate([part[:, :128] for part in rows] + [left], axis=0)


def features(got_ref, core, m, e):
    blocks = []
    for half in (core, 1 - core):
        parts = []
        for h in range(2):
            main = got_ref[2 * half + h, :, m * PACK + e * R : m * PACK + (e + 1) * R, :]
            left = got_ref[2 * half + h, :, m * PACK + 2 * R : (m + 1) * PACK, :]
            parts.append(main.reshape(ZH * X * R, 128))
            parts.append(left.reshape(ZH * X * R, 128)[:, e * 64 : (e + 1) * 64])
        blocks.append(jnp.concatenate(parts, axis=1))
    return jnp.concatenate(blocks, axis=0)


def forward_kernel(core_ref, got_ref, gate_ref, up_ref, down_ref, keep_ref, send_ref):
    core = core_ref[0]
    for e in range(2):
        rows = features(got_ref, core, 0, e)
        cot = features(got_ref, core, 1, e)
        parts = (
            dot(rows, gate_ref[e], ((1,), (0,))),
            dot(rows, up_ref[e], ((1,), (0,))),
            dot(cot, down_ref[e], ((1,), (1,))),
        )
        for t, part in enumerate(parts):
            part = part.astype(BF16).reshape(C, X, ZH * R, 512)
            keep_ref[:, 2 * t + e] = part[0]
            send_ref[:, 2 * t + e] = part[1]


def all_rows(mine_ref, other_ref, t, e):
    return jnp.concatenate(
        [ref[:, 2 * t + e].reshape(ZH * X * R, 512) for ref in (mine_ref, other_ref)], axis=0
    )


def back_kernel(core_ref, mine_ref, other_ref, gate_ref, up_ref, out_ref):
    core = core_ref[0]
    terms = []
    for e in range(2):
        grad_gate = all_rows(mine_ref, other_ref, 1, e)
        grad_up = all_rows(mine_ref, other_ref, 2, e)
        term = dot(grad_gate, gate_ref[e], ((1,), (1,))) + dot(grad_up, up_ref[e], ((1,), (1,)))
        terms.append(term.astype(BF16))
    for at, half in enumerate((core, 1 - core)):
        for h in range(2):
            rows = slice(at * ZH * X * R, (at + 1) * ZH * X * R)
            here = [term[rows, h * HALF : (h + 1) * HALF] for term in terms]
            for e in range(2):
                main = here[e][:, :128].reshape(ZH * X, R, 128)
                out_ref[2 * half + h, :, e * R : (e + 1) * R, :] = main
            left = jnp.concatenate([part[:, 128:] for part in here], axis=1)
            out_ref[2 * half + h, :, 2 * R :, :] = left.reshape(ZH * X, R, 128)


def weight_kernel(core_ref, got_ref, mine_ref, other_ref, gate_out, up_out, down_out):
    core = core_ref[0]
    for e in range(2):
        count = sum(
            jnp.sum(got_ref[2 * half, :, 2 * PACK :, :][:, :, e * 64 : (e + 1) * 64].astype(F32))
            for half in range(2)
        )
        scale = 1.0 / jnp.full((1, 512), count, F32)
        rows = features(got_ref, core, 0, e)
        cot = features(got_ref, core, 1, e)
        hidden, grad_gate, grad_up = (all_rows(mine_ref, other_ref, t, e) for t in range(3))
        gate_out[e] = (dot(rows, grad_gate, ((0,), (0,))) * scale).astype(BF16)
        up_out[e] = (dot(rows, grad_up, ((0,), (0,))) * scale).astype(BF16)
        down_out[e] = (dot(hidden, cot, ((0,), (0,))) * scale[:, :384]).astype(BF16)


def place_kernel(rows_ref, slot_ref, out_ref):
    spot = lax.broadcasted_iota(jnp.int32, (64, R), 0)
    total = jnp.zeros((64, HALF), F32)
    left = rows_ref[2 * R :, :]
    for e in range(2):
        one_hot = (spot == slot_ref[e : e + 1, :]).astype(BF16)
        rows = [rows_ref[e * R : (e + 1) * R, :], left[:, e * 64 : (e + 1) * 64]]
        total = total + dot(one_hot, jnp.concatenate(rows, axis=1), ((1,), (0,)))
    out_ref[...] = total.astype(BF16)


VM = pl.BlockSpec(memory_space=pltpu.VMEM)
SM = pl.BlockSpec(memory_space=pltpu.SMEM)
HB = pl.BlockSpec(memory_space=pltpu.HBM)


def in_vmem(x):
    return pltpu.with_memory_space_constraint(x, pltpu.VMEM)


def local(kernel, specs, outs, name, stay=True, scratch=()):
    if stay:
        shapes = [pltpu.VMEM(o, BF16) for o in outs]
    else:
        shapes = [jax.ShapeDtypeStruct(o, BF16) for o in outs]
    return pl.pallas_call(
        kernel,
        in_specs=specs,
        out_specs=[VM] * len(outs),
        out_shape=shapes,
        scratch_shapes=scratch,
        compiler_params=pltpu.CompilerParams(vmem_limit_bytes=16 << 20),
        name=name,
    )


def on_device(
    tokens, cotangent, gate_proj, up_proj, down_proj, slot_tokens, gate_weights, live_counts
):
    core = lax.axis_index("c").astype(jnp.int32).reshape(1)
    gate_proj, up_proj, down_proj = (in_vmem(w) for w in (gate_proj, up_proj, down_proj))
    scratch = [
        pltpu.VMEM(tokens.shape, BF16),
        pltpu.VMEM(cotangent.shape, BF16),
        pltpu.VMEM(slot_tokens.shape, jnp.int32),
        pltpu.VMEM(gate_weights.shape, F32),
        pltpu.SMEM((2,), jnp.int32),
        pltpu.SemaphoreType.DMA((5,)),
    ]
    (message,) = local(pick_kernel, [HB] * 5, [(MESSAGE, 128)], "pick", scratch=scratch)(
        *(
            pltpu.with_memory_space_constraint(a, pltpu.HBM)
            for a in (tokens, cotangent, slot_tokens, gate_weights, live_counts.reshape(2))
        )
    )
    message = lax.ppermute(message, EVERY, outward())
    copies = jnp.broadcast_to(message[None], (ZL, MESSAGE, 128))
    column = lax.all_to_all(copies, "zl", 0, 0, tiled=True)
    got = in_vmem(lax.all_gather(column, "y", axis=0, tiled=False))

    stage = (X, 6, ZH * R, 512)
    keep, send = local(forward_kernel, [SM, VM, VM, VM, VM], [stage, stage], "forward")(
        core, got, gate_proj, up_proj, down_proj
    )
    swap = [(0, 1), (1, 0)]
    heard = lax.ppermute(send, "c", swap)
    paired = (keep.astype(F32) + heard.astype(F32)).astype(BF16)
    over_x = lax.all_to_all(paired, "x", 0, 0, tiled=True)
    over_x = jnp.sum(over_x.astype(F32), axis=0).astype(BF16)
    over_zh = lax.all_gather(over_x, "zh", axis=0, tiled=False)
    sums = jnp.sum(over_zh.astype(F32), axis=0)
    gate_sum, up_sum, cot_hidden = sums[0:2], sums[2:4], sums[4:6]
    sigmoid_part = jax.nn.sigmoid(gate_sum)
    hidden = gate_sum * sigmoid_part * up_sum
    grad_gate = cot_hidden * up_sum * sigmoid_part * (1.0 + gate_sum * (1.0 - sigmoid_part))
    grad_up = cot_hidden * gate_sum * sigmoid_part
    acts = jnp.concatenate([hidden, grad_gate, grad_up], axis=0).astype(BF16)
    mine = lax.all_gather(acts, "x", axis=0, tiled=False)
    other = in_vmem(lax.ppermute(mine, "c", swap))
    mine = in_vmem(mine)

    (back,) = local(back_kernel, [SM, VM, VM, VM, VM], [(C * 2, X * ZH, PACK, 128)], "back")(
        core, mine, other, gate_proj, up_proj
    )
    over_y = lax.all_to_all(back, "y", 0, 0, tiled=True)
    over_y = jnp.sum(over_y.astype(F32), axis=0).astype(BF16)
    over_zl = lax.all_to_all(over_y, "zl", 0, 0, tiled=True)
    over_zl = jnp.sum(over_zl.astype(F32), axis=0).astype(BF16)
    home = in_vmem(lax.ppermute(over_zl, EVERY, homeward()))
    grad_gate_proj, grad_up_proj, grad_down_proj = local(
        weight_kernel,
        [SM, VM, VM, VM],
        [gate_proj.shape, up_proj.shape, down_proj.shape],
        "weights",
        False,
    )(core, got, mine, other)
    (grad_tokens,) = local(place_kernel, [VM, VM], [tokens.shape], "place", False)(
        home, slot_tokens
    )
    return (grad_tokens, grad_gate_proj, grad_up_proj, grad_down_proj)


def solution(mesh):
    fine = Mesh(mesh.devices.reshape(X, ZH, C, ZL, Y), EVERY)
    in_specs = (
        P(DP, SHARD),
        P(DP, SHARD),
        P(None, DP, SHARD),
        P(None, DP, SHARD),
        P(None, SHARD, DP),
        P(None, DP),
        P(None, DP),
        P(None, DP),
    )
    out_specs = (
        P(DP, SHARD),
        P(None, DP, SHARD),
        P(None, DP, SHARD),
        P(None, SHARD, DP),
    )
    return jax.shard_map(
        on_device, mesh=fine, in_specs=in_specs, out_specs=out_specs, check_vma=False
    )
```

```python
import jax
import jax.numpy as jnp
from jax import lax
from jax.experimental import pallas as pl
from jax.experimental.pallas import tpu as pltpu
from jax.sharding import Mesh, PartitionSpec as P

X, ZH, C, ZL, Y = 4, 2, 2, 8, 4
DP = ("x", "zh", "c")
SHARD = ("zl", "y")
EVERY = DP + SHARD
N_SHARD = ZL * Y
HALF = 192
R = 16
PACK = 3 * R
MESSAGE = 2 * PACK + 8
BF16 = jnp.bfloat16
F32 = jnp.float32


def ring(a, b, n):
    return min((a - b) % n, (b - a) % n)


def columns(zl):
    x_here, zh_here = divmod(zl, ZH)
    by_reach = sorted(range(ZL), key=lambda p: (abs(p - zl), p))
    by_ring = sorted(range(X), key=lambda x: (-ring(x, x_here, X), x))
    near = {(x, zh_here): p for x, p in zip(by_ring, by_reach[:4])}
    far = {(x, 1 - zh_here): p for x, p in zip(by_ring, by_reach[:3:-1])}
    return near | far


def outward():
    pairs = []
    for k in range(X * ZH * C):
        x, zh, c = k // 4, k // 2 % 2, k % 2
        for s in range(N_SHARD):
            column = columns(s // Y)[(x, zh)]
            there, h = s // 2, s % 2
            line = s % Y if c == 0 else (s % Y // 2 * 2 + 3 - h) % Y
            pairs.append((k * N_SHARD + s, there * N_SHARD + column * Y + line))
    return pairs


def code_of(zl):
    return sum(p << 3 * (ZH * x + zh) for (x, zh), p in columns(zl).items())


class Slots:
    def __init__(self, dp_ref):
        self.core = dp_ref[0] & 1
        zl = dp_ref[0] >> 1
        self.code = sum(jnp.where(zl == i, code_of(i), 0) for i in range(ZL))

    def halves(self):
        return (self.core, 1 - self.core)

    def column(self, j):
        return (self.code >> 3 * j) & 7

    def line(self, half, h):
        return jnp.where(half == 0, 2 * self.core + h, (2 * self.core + 3 - h) & 3)


def homeward():
    return [(there, here) for here, there in outward()]


def dot(a, b, dims):
    return lax.dot_general(a, b, (dims, ((), ())), preferred_element_type=F32)


def as_column(row):
    n = row.shape[1]
    eye = lax.broadcasted_iota(jnp.int32, (n, n), 0) == lax.broadcasted_iota(jnp.int32, (n, n), 1)
    return jnp.sum(jnp.where(eye, jnp.broadcast_to(row, (n, n)), 0), axis=1, keepdims=True)


def pick_kernel(
    tok_hbm, cot_hbm, slot_hbm, gate_hbm, live_hbm, out_ref, tok, cot, slots, gates, live, sems
):
    moves = [
        pltpu.make_async_copy(source, target, sems.at[i])
        for i, (source, target) in enumerate(
            (
                (slot_hbm, slots),
                (gate_hbm, gates),
                (live_hbm, live),
                (tok_hbm, tok),
                (cot_hbm, cot),
            )
        )
    ]
    for move in moves:
        move.start()
    for move in moves:
        move.wait()
    spot = lax.broadcasted_iota(jnp.int32, (R, 64), 1)
    row = lax.broadcasted_iota(jnp.int32, (R, 1), 0)
    one_hot = [(as_column(slots[e : e + 1, :]) == spot).astype(BF16) for e in range(2)]
    scale = [jnp.where(row < live[e], as_column(gates[e : e + 1, :]), 0.0) for e in range(2)]
    for m, in_ref in enumerate((tok, cot)):
        values = in_ref[...]
        rows = [dot(one_hot[e], values, ((1,), (0,))) for e in range(2)]
        if m == 1:
            rows = [rows[e] * scale[e] for e in range(2)]
        out_ref[m * PACK : (m + 1) * PACK, :] = packed([part.astype(BF16) for part in rows])
    lane = lax.broadcasted_iota(jnp.int32, (8, 128), 1)
    line = lax.broadcasted_iota(jnp.int32, (8, 128), 0)
    note = jnp.where(lane == 0, live[0], 0) + jnp.where(lane == 64, live[1], 0)
    out_ref[2 * PACK :, :] = jnp.where(line == 0, note, 0).astype(F32).astype(BF16)


def packed(rows):
    left = jnp.concatenate([part[:, 128:] for part in rows], axis=1)
    return jnp.concatenate([part[:, :128] for part in rows] + [left], axis=0)


def features(got_ref, slots, m, e):
    blocks = []
    for half in slots.halves():
        lines = [slots.line(half, h) for h in range(2)]
        for j in range(ZH * X):
            parts = []
            for line in lines:
                at = got_ref.at[line, slots.column(j)]
                parts.append(at[m * PACK + e * R : m * PACK + (e + 1) * R, :])
                left = at[m * PACK + 2 * R : (m + 1) * PACK, :]
                parts.append(left[:, e * 64 : (e + 1) * 64])
            blocks.append(jnp.concatenate(parts, axis=1))
    return jnp.concatenate(blocks, axis=0)


def forward_kernel(
    dp_ref, got_ref, gate_ref, up_ref, down_hbm, keep_ref, send_ref, down_ref, sem
):
    move = pltpu.make_async_copy(down_hbm, down_ref, sem)
    move.start()
    slots = Slots(dp_ref)

    def give(t, e, part):
        part = part.astype(BF16).reshape(C, X, ZH * R, 512)
        keep_ref[:, 2 * t + e] = part[0]
        send_ref[:, 2 * t + e] = part[1]

    for e in range(2):
        rows = features(got_ref, slots, 0, e)
        give(0, e, dot(rows, gate_ref[e], ((1,), (0,))))
        give(1, e, dot(rows, up_ref[e], ((1,), (0,))))
    move.wait()
    for e in range(2):
        give(2, e, dot(features(got_ref, slots, 1, e), down_ref[e], ((1,), (1,))))


def all_rows(mine_ref, other_ref, t, e):
    return jnp.concatenate(
        [ref[:, 2 * t + e].reshape(ZH * X * R, 512) for ref in (mine_ref, other_ref)], axis=0
    )


def back_kernel(dp_ref, mine_ref, other_ref, gate_ref, up_ref, out_ref):
    slots = Slots(dp_ref)
    terms = []
    for e in range(2):
        grad_gate = all_rows(mine_ref, other_ref, 1, e)
        grad_up = all_rows(mine_ref, other_ref, 2, e)
        term = dot(grad_gate, gate_ref[e], ((1,), (1,))) + dot(grad_up, up_ref[e], ((1,), (1,)))
        terms.append(term.astype(BF16))
    for i, half in enumerate(slots.halves()):
        for h in range(2):
            line = slots.line(half, h)
            for j in range(ZH * X):
                first = (i * ZH * X + j) * R
                rows = [
                    term[first : first + R, h * HALF : (h + 1) * HALF] for term in terms
                ]
                out_ref[line, slots.column(j)] = packed(rows)


def weight_kernel(dp_ref, got_ref, mine_ref, other_ref, gate_out, up_out, down_out):
    slots = Slots(dp_ref)
    notes = got_ref[:, :, 2 * PACK :, :].astype(F32).reshape(Y * ZL * 8, 128)
    for e in range(2):
        count = 0.5 * jnp.sum(notes[:, e * 64 : (e + 1) * 64])
        scale = 1.0 / jnp.full((1, 512), count, F32)
        rows = features(got_ref, slots, 0, e)
        cot = features(got_ref, slots, 1, e)
        hidden, grad_gate, grad_up = (all_rows(mine_ref, other_ref, t, e) for t in range(3))
        gate_out[e] = (dot(rows, grad_gate, ((0,), (0,))) * scale).astype(BF16)
        up_out[e] = (dot(rows, grad_up, ((0,), (0,))) * scale).astype(BF16)
        down_out[e] = (dot(hidden, cot, ((0,), (0,))) * scale[:, :384]).astype(BF16)


def place_kernel(rows_ref, slot_ref, out_ref):
    spot = lax.broadcasted_iota(jnp.int32, (64, R), 0)
    total = jnp.zeros((64, HALF), F32)
    left = rows_ref[2 * R :, :]
    for e in range(2):
        one_hot = (spot == slot_ref[e : e + 1, :]).astype(BF16)
        rows = [rows_ref[e * R : (e + 1) * R, :], left[:, e * 64 : (e + 1) * 64]]
        total = total + dot(one_hot, jnp.concatenate(rows, axis=1), ((1,), (0,)))
    out_ref[...] = total.astype(BF16)


VM = pl.BlockSpec(memory_space=pltpu.VMEM)
SM = pl.BlockSpec(memory_space=pltpu.SMEM)
HB = pl.BlockSpec(memory_space=pltpu.HBM)


def in_vmem(x):
    return pltpu.with_memory_space_constraint(x, pltpu.VMEM)


def in_hbm(x):
    return pltpu.with_memory_space_constraint(x, pltpu.HBM)


def local(kernel, specs, outs, name, stay=True, scratch=()):
    if stay:
        shapes = [pltpu.VMEM(o, BF16) for o in outs]
    else:
        shapes = [jax.ShapeDtypeStruct(o, BF16) for o in outs]
    return pl.pallas_call(
        kernel,
        in_specs=specs,
        out_specs=[VM] * len(outs),
        out_shape=shapes,
        scratch_shapes=scratch,
        compiler_params=pltpu.CompilerParams(vmem_limit_bytes=16 << 20),
        name=name,
    )


def on_device(
    tokens, cotangent, gate_proj, up_proj, down_proj, slot_tokens, gate_weights, live_counts
):
    dp = lax.axis_index(DP).astype(jnp.int32).reshape(1)
    gate_proj, up_proj = in_vmem(gate_proj), in_vmem(up_proj)
    scratch = [
        pltpu.VMEM(tokens.shape, BF16),
        pltpu.VMEM(cotangent.shape, BF16),
        pltpu.VMEM(slot_tokens.shape, jnp.int32),
        pltpu.VMEM(gate_weights.shape, F32),
        pltpu.SMEM((2,), jnp.int32),
        pltpu.SemaphoreType.DMA((5,)),
    ]
    (message,) = local(pick_kernel, [HB] * 5, [(MESSAGE, 128)], "pick", scratch=scratch)(
        *(
            in_hbm(a)
            for a in (tokens, cotangent, slot_tokens, gate_weights, live_counts.reshape(2))
        )
    )
    message = lax.ppermute(message, EVERY, outward())
    copies = jnp.broadcast_to(message[None], (ZL, MESSAGE, 128))
    column = lax.all_to_all(copies, "zl", 0, 0, tiled=True)
    got = in_vmem(lax.all_gather(column, "y", axis=0, tiled=False))

    stage = (X, 6, ZH * R, 512)
    scratch = [pltpu.VMEM(down_proj.shape, BF16), pltpu.SemaphoreType.DMA]
    keep, send = local(
        forward_kernel, [SM, VM, VM, VM, HB], [stage, stage], "forward", scratch=scratch
    )(dp, got, gate_proj, up_proj, in_hbm(down_proj))
    swap = [(0, 1), (1, 0)]
    heard = lax.ppermute(send, "c", swap)
    paired = (keep.astype(F32) + heard.astype(F32)).astype(BF16)
    over_x = lax.all_to_all(paired, "x", 0, 0, tiled=True)
    over_x = jnp.sum(over_x.astype(F32), axis=0).astype(BF16)
    over_zh = lax.all_gather(over_x, "zh", axis=0, tiled=False)
    sums = jnp.sum(over_zh.astype(F32), axis=0)
    gate_sum, up_sum, cot_hidden = sums[0:2], sums[2:4], sums[4:6]
    sigmoid_part = jax.nn.sigmoid(gate_sum)
    hidden = gate_sum * sigmoid_part * up_sum
    grad_gate = cot_hidden * up_sum * sigmoid_part * (1.0 + gate_sum * (1.0 - sigmoid_part))
    grad_up = cot_hidden * gate_sum * sigmoid_part
    acts = jnp.concatenate([hidden, grad_gate, grad_up], axis=0).astype(BF16)
    mine = lax.all_gather(acts, "x", axis=0, tiled=False)
    other = in_vmem(lax.ppermute(mine, "c", swap))
    mine = in_vmem(mine)

    (back,) = local(back_kernel, [SM, VM, VM, VM, VM], [(C * 2, X * ZH, PACK, 128)], "back")(
        dp, mine, other, gate_proj, up_proj
    )
    over_y = lax.all_to_all(back, "y", 0, 0, tiled=True)
    over_y = jnp.sum(over_y.astype(F32), axis=0).astype(BF16)
    over_zl = lax.all_to_all(over_y, "zl", 0, 0, tiled=True)
    over_zl = jnp.sum(over_zl.astype(F32), axis=0).astype(BF16)
    home = in_vmem(lax.ppermute(over_zl, EVERY, homeward()))
    grad_gate_proj, grad_up_proj, grad_down_proj = local(
        weight_kernel,
        [SM, VM, VM, VM],
        [gate_proj.shape, up_proj.shape, down_proj.shape],
        "weights",
        False,
    )(dp, got, mine, other)
    (grad_tokens,) = local(place_kernel, [VM, VM], [tokens.shape], "place", False)(
        home, slot_tokens
    )
    return (grad_tokens, grad_gate_proj, grad_up_proj, grad_down_proj)


def solution(mesh):
    fine = Mesh(mesh.devices.reshape(X, ZH, C, ZL, Y), EVERY)
    in_specs = (
        P(DP, SHARD),
        P(DP, SHARD),
        P(None, DP, SHARD),
        P(None, DP, SHARD),
        P(None, SHARD, DP),
        P(None, DP),
        P(None, DP),
        P(None, DP),
    )
    out_specs = (
        P(DP, SHARD),
        P(None, DP, SHARD),
        P(None, DP, SHARD),
        P(None, SHARD, DP),
    )
    return jax.shard_map(
        on_device, mesh=fine, in_specs=in_specs, out_specs=out_specs, check_vma=False
    )
```

```python
import jax
import jax.numpy as jnp
from jax import lax
from jax.experimental import pallas as pl
from jax.experimental.pallas import tpu as pltpu
from jax.sharding import Mesh, PartitionSpec as P

X, ZH, C, ZL, Y = 4, 2, 2, 8, 4
DP = ("x", "zh", "c")
SHARD = ("zl", "y")
EVERY = DP + SHARD
N_SHARD = ZL * Y
HALF = 192
R = 16
PACK = 3 * R
MESSAGE = 2 * PACK + 8
BF16 = jnp.bfloat16
F32 = jnp.float32


def ring(a, b, n):
    return min((a - b) % n, (b - a) % n)


def columns(zl):
    x_here, zh_here = divmod(zl, ZH)
    by_reach = sorted(range(ZL), key=lambda p: (abs(p - zl), p))
    by_ring = sorted(range(X), key=lambda x: (-ring(x, x_here, X), x))
    near = {(x, zh_here): p for x, p in zip(by_ring, by_reach[:4])}
    far = {(x, 1 - zh_here): p for x, p in zip(by_ring, by_reach[:3:-1])}
    return near | far


def outward():
    pairs = []
    for k in range(X * ZH * C):
        x, zh, c = k // 4, k // 2 % 2, k % 2
        for s in range(N_SHARD):
            zl, y = divmod(s, Y)
            there = zl * C + c
            pairs.append((k * N_SHARD + s, there * N_SHARD + columns(zl)[(x, zh)] * Y + y))
    return pairs


def code_of(zl):
    return sum(p << 3 * (ZH * x + zh) for (x, zh), p in columns(zl).items())


class Slots:
    def __init__(self, dp_ref):
        self.core = dp_ref[0] & 1
        zl = dp_ref[0] >> 1
        self.code = sum(jnp.where(zl == i, code_of(i), 0) for i in range(ZL))

    def halves(self):
        return (self.core, 1 - self.core)

    def column(self, j):
        return (self.code >> 3 * j) & 7


def homeward():
    return [(there, here) for here, there in outward()]


def dot(a, b, dims):
    return lax.dot_general(a, b, (dims, ((), ())), preferred_element_type=F32)


def as_column(row):
    n = row.shape[1]
    eye = lax.broadcasted_iota(jnp.int32, (n, n), 0) == lax.broadcasted_iota(jnp.int32, (n, n), 1)
    return jnp.sum(jnp.where(eye, jnp.broadcast_to(row, (n, n)), 0), axis=1, keepdims=True)


def pick_kernel(
    tok_hbm, cot_hbm, slot_hbm, gate_hbm, live_hbm, out_ref, tok, cot, slots, gates, live, sems
):
    moves = [
        pltpu.make_async_copy(source, target, sems.at[i])
        for i, (source, target) in enumerate(
            (
                (slot_hbm, slots),
                (gate_hbm, gates),
                (live_hbm, live),
                (tok_hbm, tok),
                (cot_hbm, cot),
            )
        )
    ]
    for move in moves:
        move.start()
    for move in moves:
        move.wait()
    spot = lax.broadcasted_iota(jnp.int32, (R, 64), 1)
    row = lax.broadcasted_iota(jnp.int32, (R, 1), 0)
    one_hot = [(as_column(slots[e : e + 1, :]) == spot).astype(BF16) for e in range(2)]
    scale = [jnp.where(row < live[e], as_column(gates[e : e + 1, :]), 0.0) for e in range(2)]
    for m, in_ref in enumerate((tok, cot)):
        values = in_ref[...]
        rows = [dot(one_hot[e], values, ((1,), (0,))) for e in range(2)]
        if m == 1:
            rows = [rows[e] * scale[e] for e in range(2)]
        out_ref[m * PACK : (m + 1) * PACK, :] = packed([part.astype(BF16) for part in rows])
    lane = lax.broadcasted_iota(jnp.int32, (8, 128), 1)
    line = lax.broadcasted_iota(jnp.int32, (8, 128), 0)
    note = jnp.where(lane == 0, live[0], 0) + jnp.where(lane == 64, live[1], 0)
    out_ref[2 * PACK :, :] = jnp.where(line == 0, note, 0).astype(F32).astype(BF16)


def packed(rows):
    left = jnp.concatenate([part[:, 128:] for part in rows], axis=1)
    return jnp.concatenate([part[:, :128] for part in rows] + [left], axis=0)


def features(at, slots, m, e):
    blocks = []
    for j in range(ZH * X):
        parts = []
        for h in range(2):
            block = at(h, slots.column(j))
            parts.append(block[m * PACK + e * R : m * PACK + (e + 1) * R, :])
            left = block[m * PACK + 2 * R : (m + 1) * PACK, :]
            parts.append(left[:, e * 64 : (e + 1) * 64])
        blocks.append(jnp.concatenate(parts, axis=1))
    return jnp.concatenate(blocks, axis=0)


def lines_of(got_ref, half):
    return lambda h, column: got_ref.at[2 * half + h, column]


def forward_kernel(dp_ref, got_ref, *refs):
    *weights, out_ref, loan_ref, down_a, down_b, sems = refs
    moves = [
        pltpu.make_async_copy(weights[4 + i], target, sems.at[i])
        for i, target in enumerate((down_a, down_b))
    ]
    for move in moves:
        move.start()
    slots = Slots(dp_ref)

    def give(t, e, rows, pair, dims):
        part = dot(rows[0], pair[0][e], dims) + dot(rows[1], pair[1][e], dims)
        out_ref[:, 2 * t + e] = part.astype(BF16).reshape(X, ZH * R, 512)

    def both(m, e):
        return [features(lines_of(got_ref, half), slots, m, e) for half in slots.halves()]

    for e in range(2):
        rows = both(0, e)
        give(0, e, rows, weights[0:2], ((1,), (0,)))
        give(1, e, rows, weights[2:4], ((1,), (0,)))
    for h in range(2):
        loan_ref[h] = got_ref[2 * (1 - slots.core) + h]
    for move in moves:
        move.wait()
    for e in range(2):
        give(2, e, both(1, e), (down_a, down_b), ((1,), (1,)))


def all_rows(refs, t, e):
    return jnp.concatenate([ref[:, 2 * t + e].reshape(ZH * X * R, 512) for ref in refs], axis=0)


def back_kernel(dp_ref, mine_ref, *refs):
    *weights, out_ref = refs
    slots = Slots(dp_ref)
    grads = [[all_rows((mine_ref,), t, e) for t in (1, 2)] for e in range(2)]
    for i, half in enumerate(slots.halves()):
        terms = [
            sum(dot(grads[e][t], weights[2 * t + i][e], ((1,), (1,))) for t in range(2)).astype(BF16)
            for e in range(2)
        ]
        for h in range(2):
            for j in range(ZH * X):
                rows = [term[j * R : (j + 1) * R, h * HALF : (h + 1) * HALF] for term in terms]
                out_ref[2 * half + h, slots.column(j)] = packed(rows)


def weight_kernel(dp_ref, got_ref, lent_ref, mine_ref, other_ref, gate_out, up_out, down_out):
    slots = Slots(dp_ref)
    notes = [ref[0, :, 2 * PACK :, :].astype(F32).reshape(ZL * 8, 128) for ref in (got_ref, lent_ref)]
    notes = jnp.concatenate(notes, axis=0)
    acts = (mine_ref, other_ref)
    for e in range(2):
        scale = 1.0 / jnp.full((1, 512), jnp.sum(notes[:, e * 64 : (e + 1) * 64]), F32)
        rows, cot = (
            jnp.concatenate(
                [
                    features(lines_of(got_ref, slots.core), slots, m, e),
                    features(lines_of(lent_ref, 0), slots, m, e),
                ],
                axis=0,
            )
            for m in range(2)
        )
        hidden, grad_gate, grad_up = (all_rows(acts, t, e) for t in range(3))
        gate_out[e] = (dot(rows, grad_gate, ((0,), (0,))) * scale).astype(BF16)
        up_out[e] = (dot(rows, grad_up, ((0,), (0,))) * scale).astype(BF16)
        down_out[e] = (dot(hidden, cot, ((0,), (0,))) * scale[:, :384]).astype(BF16)


def place_kernel(rows_ref, slot_ref, out_ref):
    spot = lax.broadcasted_iota(jnp.int32, (64, R), 0)
    total = jnp.zeros((64, HALF), F32)
    left = rows_ref[2 * R :, :]
    for e in range(2):
        one_hot = (spot == slot_ref[e : e + 1, :]).astype(BF16)
        rows = [rows_ref[e * R : (e + 1) * R, :], left[:, e * 64 : (e + 1) * 64]]
        total = total + dot(one_hot, jnp.concatenate(rows, axis=1), ((1,), (0,)))
    out_ref[...] = total.astype(BF16)


VM = pl.BlockSpec(memory_space=pltpu.VMEM)
SM = pl.BlockSpec(memory_space=pltpu.SMEM)
HB = pl.BlockSpec(memory_space=pltpu.HBM)


def in_vmem(x):
    return pltpu.with_memory_space_constraint(x, pltpu.VMEM)


def in_hbm(x):
    return pltpu.with_memory_space_constraint(x, pltpu.HBM)


def local(kernel, specs, outs, stay=True, scratch=()):
    if stay:
        shapes = [pltpu.VMEM(o, BF16) for o in outs]
    else:
        shapes = [jax.ShapeDtypeStruct(o, BF16) for o in outs]
    return pl.pallas_call(
        kernel,
        in_specs=specs,
        out_specs=[VM] * len(outs),
        out_shape=shapes,
        scratch_shapes=scratch,
        compiler_params=pltpu.CompilerParams(vmem_limit_bytes=16 << 20),
    )


def layer(
    tokens, cotangent, gate_proj, up_proj, down_proj, slot_tokens, gate_weights, live_counts
):
    dp = lax.axis_index(DP).astype(jnp.int32).reshape(1)
    scratch = [
        pltpu.VMEM(tokens.shape, BF16),
        pltpu.VMEM(cotangent.shape, BF16),
        pltpu.VMEM(slot_tokens.shape, jnp.int32),
        pltpu.VMEM(gate_weights.shape, F32),
        pltpu.SMEM((2,), jnp.int32),
        pltpu.SemaphoreType.DMA((5,)),
    ]
    (message,) = local(pick_kernel, [HB] * 5, [(MESSAGE, 128)], scratch=scratch)(
        *(
            in_hbm(a)
            for a in (tokens, cotangent, slot_tokens, gate_weights, live_counts.reshape(2))
        )
    )
    swap = [(0, 1), (1, 0)]
    message = lax.ppermute(message, EVERY, outward())
    pairs = [
        (place(w), place(lax.ppermute(w, "c", swap)))
        for w, place in ((gate_proj, in_vmem), (up_proj, in_vmem), (down_proj, in_hbm))
    ]
    copies = jnp.broadcast_to(message[None], (ZL, MESSAGE, 128))
    column = lax.all_to_all(copies, "zl", 0, 0, tiled=True)
    got = in_vmem(lax.all_gather(column, "y", axis=0, tiled=False))

    parts, loan = local(
        forward_kernel,
        [SM] + [VM] * 5 + [HB] * 2,
        [(X, 6, ZH * R, 512), (2, ZL, MESSAGE, 128)],
        scratch=[pltpu.VMEM(down_proj.shape, BF16)] * 2 + [pltpu.SemaphoreType.DMA((2,))],
    )(dp, got, *pairs[0], *pairs[1], *pairs[2])
    lent = lax.ppermute(loan, "c", swap)
    over_x = lax.all_to_all(parts, "x", 0, 0, tiled=True)
    over_x = jnp.sum(over_x.astype(F32), axis=0).astype(BF16)
    over_zh = lax.all_gather(over_x, "zh", axis=0, tiled=False)
    sums = jnp.sum(over_zh.astype(F32), axis=0)
    gate_sum, up_sum, cot_hidden = sums[0:2], sums[2:4], sums[4:6]
    sigmoid_part = jax.nn.sigmoid(gate_sum)
    hidden = gate_sum * sigmoid_part * up_sum
    grad_gate = cot_hidden * up_sum * sigmoid_part * (1.0 + gate_sum * (1.0 - sigmoid_part))
    grad_up = cot_hidden * gate_sum * sigmoid_part
    acts = jnp.concatenate([hidden, grad_gate, grad_up], axis=0).astype(BF16)
    mine = lax.all_gather(acts, "x", axis=0, tiled=False)
    other = lax.ppermute(mine, "c", swap)
    mine = in_vmem(mine)

    (back,) = local(back_kernel, [SM] + [VM] * 5, [(Y, ZL, PACK, 128)], False)(
        dp, mine, *pairs[0], *pairs[1]
    )
    over_y = lax.all_to_all(back, "y", 0, 0, tiled=True)
    over_y = jnp.sum(over_y.astype(F32), axis=0).astype(BF16)
    over_zl = lax.all_to_all(over_y, "zl", 0, 0, tiled=True)
    over_zl = jnp.sum(over_zl.astype(F32), axis=0).astype(BF16)
    home = lax.ppermute(over_zl, EVERY, homeward())
    home = in_vmem(home)
    grad_gate_proj, grad_up_proj, grad_down_proj = local(
        weight_kernel,
        [SM, VM, VM, VM, VM],
        [gate_proj.shape, up_proj.shape, down_proj.shape],
        False,
    )(dp, got, lent, mine, other)
    (grad_tokens,) = local(place_kernel, [VM, VM], [tokens.shape], False)(home, slot_tokens)
    return (grad_tokens, grad_gate_proj, grad_up_proj, grad_down_proj)


def solution(mesh):
    fine = Mesh(mesh.devices.reshape(X, ZH, C, ZL, Y), EVERY)
    in_specs = (
        P(DP, SHARD),
        P(DP, SHARD),
        P(None, DP, SHARD),
        P(None, DP, SHARD),
        P(None, SHARD, DP),
        P(None, DP),
        P(None, DP),
        P(None, DP),
    )
    out_specs = (
        P(DP, SHARD),
        P(None, DP, SHARD),
        P(None, DP, SHARD),
        P(None, SHARD, DP),
    )
    return jax.shard_map(layer, mesh=fine, in_specs=in_specs, out_specs=out_specs, check_vma=False)
```

```python
import jax
import jax.numpy as jnp
from jax import lax
from jax.experimental import pallas as pl
from jax.experimental.pallas import tpu as pltpu
from jax.sharding import Mesh, PartitionSpec as P

X, ZH, C, ZL, Y = 4, 2, 2, 8, 4
DP = ("x", "zh", "c")
SHARD = ("zl", "y")
EVERY = DP + SHARD
N_SHARD = ZL * Y
HALF = 192
R = 16
PACK = 3 * R
MESSAGE = 2 * PACK + 8
BF16 = jnp.bfloat16
F32 = jnp.float32


def ring(a, b, n):
    return min((a - b) % n, (b - a) % n)


def columns(zl):
    x_here, zh_here = divmod(zl, ZH)
    by_reach = sorted(range(ZL), key=lambda p: (abs(p - zl), p))
    by_ring = sorted(range(X), key=lambda x: (-ring(x, x_here, X), x))
    near = {(x, zh_here): p for x, p in zip(by_ring, by_reach[:4])}
    far = {(x, 1 - zh_here): p for x, p in zip(by_ring, by_reach[:3:-1])}
    return near | far


def outward():
    pairs = []
    for k in range(X * ZH * C):
        x, zh, c = k // 4, k // 2 % 2, k % 2
        for s in range(N_SHARD):
            zl, y = divmod(s, Y)
            there = zl * C + c
            pairs.append((k * N_SHARD + s, there * N_SHARD + columns(zl)[(x, zh)] * Y + y))
    return pairs


def code_of(zl):
    return sum(p << 3 * (ZH * x + zh) for (x, zh), p in columns(zl).items())


class Slots:
    def __init__(self, dp_ref):
        self.core = dp_ref[0] & 1
        zl = dp_ref[0] >> 1
        self.code = sum(jnp.where(zl == i, code_of(i), 0) for i in range(ZL))

    def halves(self):
        return (self.core, 1 - self.core)

    def column(self, j):
        return (self.code >> 3 * j) & 7


def homeward():
    return [(there, here) for here, there in outward()]


def dot(a, b, dims):
    return lax.dot_general(a, b, (dims, ((), ())), preferred_element_type=F32)


def as_column(row):
    n = row.shape[1]
    eye = lax.broadcasted_iota(jnp.int32, (n, n), 0) == lax.broadcasted_iota(jnp.int32, (n, n), 1)
    return jnp.sum(jnp.where(eye, jnp.broadcast_to(row, (n, n)), 0), axis=1, keepdims=True)


def pick_kernel(
    tok_hbm, cot_hbm, slot_hbm, gate_hbm, live_hbm, out_ref, tok, cot, slots, gates, live, sems
):
    moves = [
        pltpu.make_async_copy(source, target, sems.at[i])
        for i, (source, target) in enumerate(
            (
                (slot_hbm, slots),
                (gate_hbm, gates),
                (live_hbm, live),
                (tok_hbm, tok),
                (cot_hbm, cot),
            )
        )
    ]
    for move in moves:
        move.start()
    for move in moves:
        move.wait()
    spot = lax.broadcasted_iota(jnp.int32, (R, 64), 1)
    row = lax.broadcasted_iota(jnp.int32, (R, 1), 0)
    one_hot = [(as_column(slots[e : e + 1, :]) == spot).astype(BF16) for e in range(2)]
    scale = [jnp.where(row < live[e], as_column(gates[e : e + 1, :]), 0.0) for e in range(2)]
    for m, in_ref in enumerate((tok, cot)):
        values = in_ref[...]
        rows = [dot(one_hot[e], values, ((1,), (0,))) for e in range(2)]
        if m == 1:
            rows = [rows[e] * scale[e] for e in range(2)]
        out_ref[m * PACK : (m + 1) * PACK, :] = packed([part.astype(BF16) for part in rows])
    lane = lax.broadcasted_iota(jnp.int32, (8, 128), 1)
    line = lax.broadcasted_iota(jnp.int32, (8, 128), 0)
    note = jnp.where(lane == 0, live[0], 0) + jnp.where(lane == 64, live[1], 0)
    out_ref[2 * PACK :, :] = jnp.where(line == 0, note, 0).astype(F32).astype(BF16)


def packed(rows):
    left = jnp.concatenate([part[:, 128:] for part in rows], axis=1)
    return jnp.concatenate([part[:, :128] for part in rows] + [left], axis=0)


def features(at, slots, m, e):
    blocks = []
    for j in range(ZH * X):
        parts = []
        for h in range(2):
            block = at(h, slots.column(j))
            parts.append(block[m * PACK + e * R : m * PACK + (e + 1) * R, :])
            left = block[m * PACK + 2 * R : (m + 1) * PACK, :]
            parts.append(left[:, e * 64 : (e + 1) * 64])
        blocks.append(jnp.concatenate(parts, axis=1))
    return jnp.concatenate(blocks, axis=0)


def lines_of(got_ref, half):
    return lambda h, column: got_ref.at[2 * half + h, column]


def forward_kernel(
    dp_ref,
    got_ref,
    gate_ref,
    up_ref,
    gate_hbm,
    up_hbm,
    down_hbm,
    far_down_hbm,
    out_ref,
    loan_ref,
    far_gate,
    far_up,
    down_ref,
    far_down,
    sems,
):
    moves = [
        pltpu.make_async_copy(source, target, sems.at[i])
        for i, (source, target) in enumerate(
            (
                (gate_hbm, far_gate),
                (up_hbm, far_up),
                (down_hbm, down_ref),
                (far_down_hbm, far_down),
            )
        )
    ]
    for move in moves:
        move.start()
    slots = Slots(dp_ref)

    def give(t, e, part):
        out_ref[:, 2 * t + e] = part.astype(BF16).reshape(X, ZH * R, 512)

    def both(m, e):
        return [features(lines_of(got_ref, half), slots, m, e) for half in slots.halves()]

    rows = [both(0, e) for e in range(2)]
    inward = ((1,), (0,))
    near = [[dot(rows[e][0], ref[e], inward) for e in range(2)] for ref in (gate_ref, up_ref)]
    for t, ref in enumerate((far_gate, far_up)):
        moves[t].wait()
        for e in range(2):
            give(t, e, near[t][e] + dot(rows[e][1], ref[e], inward))
    for h in range(2):
        loan_ref[h] = got_ref[2 * (1 - slots.core) + h]
    moves[2].wait()
    moves[3].wait()
    for e in range(2):
        rows = both(1, e)
        across = ((1,), (1,))
        give(2, e, dot(rows[0], down_ref[e], across) + dot(rows[1], far_down[e], across))


def all_rows(refs, t, e):
    return jnp.concatenate([ref[:, 2 * t + e].reshape(ZH * X * R, 512) for ref in refs], axis=0)


def back_kernel(dp_ref, mine_ref, *refs):
    *weights, out_ref = refs
    slots = Slots(dp_ref)
    grads = [[all_rows((mine_ref,), t, e) for t in (1, 2)] for e in range(2)]
    for i, half in enumerate(slots.halves()):
        terms = [
            sum(dot(grads[e][t], weights[2 * t + i][e], ((1,), (1,))) for t in range(2)).astype(BF16)
            for e in range(2)
        ]
        for h in range(2):
            for j in range(ZH * X):
                rows = [term[j * R : (j + 1) * R, h * HALF : (h + 1) * HALF] for term in terms]
                out_ref[2 * half + h, slots.column(j)] = packed(rows)


def weight_kernel(dp_ref, got_ref, lent_ref, mine_ref, other_ref, gate_out, up_out, down_out):
    slots = Slots(dp_ref)
    notes = [ref[0, :, 2 * PACK :, :].astype(F32).reshape(ZL * 8, 128) for ref in (got_ref, lent_ref)]
    notes = jnp.concatenate(notes, axis=0)
    acts = (mine_ref, other_ref)
    for e in range(2):
        scale = 1.0 / jnp.full((1, 512), jnp.sum(notes[:, e * 64 : (e + 1) * 64]), F32)
        rows, cot = (
            jnp.concatenate(
                [
                    features(lines_of(got_ref, slots.core), slots, m, e),
                    features(lines_of(lent_ref, 0), slots, m, e),
                ],
                axis=0,
            )
            for m in range(2)
        )
        hidden, grad_gate, grad_up = (all_rows(acts, t, e) for t in range(3))
        gate_out[e] = (dot(rows, grad_gate, ((0,), (0,))) * scale).astype(BF16)
        up_out[e] = (dot(rows, grad_up, ((0,), (0,))) * scale).astype(BF16)
        down_out[e] = (dot(hidden, cot, ((0,), (0,))) * scale[:, :384]).astype(BF16)


def place_kernel(rows_ref, slot_ref, out_ref):
    spot = lax.broadcasted_iota(jnp.int32, (64, R), 0)
    total = jnp.zeros((64, HALF), F32)
    left = rows_ref[2 * R :, :]
    for e in range(2):
        one_hot = (spot == slot_ref[e : e + 1, :]).astype(BF16)
        rows = [rows_ref[e * R : (e + 1) * R, :], left[:, e * 64 : (e + 1) * 64]]
        total = total + dot(one_hot, jnp.concatenate(rows, axis=1), ((1,), (0,)))
    out_ref[...] = total.astype(BF16)


VM = pl.BlockSpec(memory_space=pltpu.VMEM)
SM = pl.BlockSpec(memory_space=pltpu.SMEM)
HB = pl.BlockSpec(memory_space=pltpu.HBM)


def in_vmem(x):
    return pltpu.with_memory_space_constraint(x, pltpu.VMEM)


def in_hbm(x):
    return pltpu.with_memory_space_constraint(x, pltpu.HBM)


def local(kernel, specs, outs, stay=True, scratch=()):
    if stay:
        shapes = [pltpu.VMEM(o, BF16) for o in outs]
    else:
        shapes = [pltpu.HBM(o, BF16) for o in outs]
    return pl.pallas_call(
        kernel,
        in_specs=specs,
        out_specs=[VM] * len(outs),
        out_shape=shapes,
        scratch_shapes=scratch,
        compiler_params=pltpu.CompilerParams(vmem_limit_bytes=16 << 20),
    )


def layer(
    tokens, cotangent, gate_proj, up_proj, down_proj, slot_tokens, gate_weights, live_counts
):
    dp = lax.axis_index(DP).astype(jnp.int32).reshape(1)
    scratch = [
        pltpu.VMEM(tokens.shape, BF16),
        pltpu.VMEM(cotangent.shape, BF16),
        pltpu.VMEM(slot_tokens.shape, jnp.int32),
        pltpu.VMEM(gate_weights.shape, F32),
        pltpu.SMEM((2,), jnp.int32),
        pltpu.SemaphoreType.DMA((5,)),
    ]
    (message,) = local(pick_kernel, [HB] * 5, [(MESSAGE, 128)], scratch=scratch)(
        *(
            in_hbm(a)
            for a in (tokens, cotangent, slot_tokens, gate_weights, live_counts.reshape(2))
        )
    )
    swap = [(0, 1), (1, 0)]
    message = lax.ppermute(message, EVERY, outward())
    far = [lax.ppermute(w, "c", swap) for w in (gate_proj, up_proj, down_proj)]
    gate, up = in_vmem(gate_proj), in_vmem(up_proj)
    copies = jnp.broadcast_to(message[None], (ZL, MESSAGE, 128))
    column = lax.all_to_all(copies, "zl", 0, 0, tiled=True)
    got = in_vmem(lax.all_gather(column, "y", axis=0, tiled=False))

    parts, loan, far_gate, far_up = local(
        forward_kernel,
        [SM] + [VM] * 3 + [HB] * 4,
        [(X, 6, ZH * R, 512), (2, ZL, MESSAGE, 128), gate.shape, up.shape],
        scratch=[pltpu.VMEM(down_proj.shape, BF16)] * 2 + [pltpu.SemaphoreType.DMA((4,))],
    )(dp, got, gate, up, *(in_hbm(w) for w in (far[0], far[1], down_proj, far[2])))
    lent = lax.ppermute(loan, "c", swap)
    over_x = lax.all_to_all(parts, "x", 0, 0, tiled=True)
    over_x = jnp.sum(over_x.astype(F32), axis=0).astype(BF16)
    over_zh = lax.all_gather(over_x, "zh", axis=0, tiled=False)
    sums = jnp.sum(over_zh.astype(F32), axis=0)
    gate_sum, up_sum, cot_hidden = sums[0:2], sums[2:4], sums[4:6]
    sigmoid_part = jax.nn.sigmoid(gate_sum)
    hidden = gate_sum * sigmoid_part * up_sum
    grad_gate = cot_hidden * up_sum * sigmoid_part * (1.0 + gate_sum * (1.0 - sigmoid_part))
    grad_up = cot_hidden * gate_sum * sigmoid_part
    acts = jnp.concatenate([hidden, grad_gate, grad_up], axis=0).astype(BF16)
    mine = lax.all_gather(acts, "x", axis=0, tiled=False)
    other = lax.ppermute(mine, "c", swap)
    mine = in_vmem(mine)

    (back,) = local(back_kernel, [SM] + [VM] * 5, [(Y, ZL, PACK, 128)], False)(
        dp, mine, gate, far_gate, up, far_up
    )
    over_y = lax.all_to_all(back, "y", 0, 0, tiled=True)
    over_y = jnp.sum(over_y.astype(F32), axis=0).astype(BF16)
    over_zl = lax.all_to_all(over_y, "zl", 0, 0, tiled=True)
    over_zl = jnp.sum(over_zl.astype(F32), axis=0).astype(BF16)
    home = lax.ppermute(over_zl, EVERY, homeward())
    home = in_vmem(home)
    grad_gate_proj, grad_up_proj, grad_down_proj = local(
        weight_kernel,
        [SM, VM, VM, VM, VM],
        [gate_proj.shape, up_proj.shape, down_proj.shape],
        False,
    )(dp, got, lent, mine, other)
    (grad_tokens,) = local(place_kernel, [VM, VM], [tokens.shape], False)(home, slot_tokens)
    return (grad_tokens, grad_gate_proj, grad_up_proj, grad_down_proj)


def solution(mesh):
    fine = Mesh(mesh.devices.reshape(X, ZH, C, ZL, Y), EVERY)
    in_specs = (
        P(DP, SHARD),
        P(DP, SHARD),
        P(None, DP, SHARD),
        P(None, DP, SHARD),
        P(None, SHARD, DP),
        P(None, DP),
        P(None, DP),
        P(None, DP),
    )
    out_specs = (
        P(DP, SHARD),
        P(None, DP, SHARD),
        P(None, DP, SHARD),
        P(None, SHARD, DP),
    )
    return jax.shard_map(layer, mesh=fine, in_specs=in_specs, out_specs=out_specs, check_vma=False)
```

```python
import jax
import jax.numpy as jnp
from jax import lax
from jax.experimental import pallas as pl
from jax.experimental.pallas import tpu as pltpu
from jax.sharding import Mesh, PartitionSpec as P

X, ZH, C, ZB, ZA, Y = 4, 2, 2, 2, 4, 4
ZL = ZB * ZA
DP = ("x", "zh", "c")
LINE = ("zb", "za")
SHARD = LINE + ("y",)
EVERY = DP + SHARD
N_SHARD = ZL * Y
HALF = 192
R = 16
PACK = 3 * R
MESSAGE = 2 * PACK + 8
BF16 = jnp.bfloat16
F32 = jnp.float32


def ring(a, b, n):
    return min((a - b) % n, (b - a) % n)


def columns(zl):
    x_here, zh_here = divmod(zl, ZH)
    by_reach = sorted(range(ZL), key=lambda p: (abs(p - zl), p))
    by_ring = sorted(range(X), key=lambda x: (-ring(x, x_here, X), x))
    near = {(x, zh_here): p for x, p in zip(by_ring, by_reach[:4])}
    far = {(x, 1 - zh_here): p for x, p in zip(by_ring, by_reach[:3:-1])}
    return near | far


def outward(flip=0):
    pairs = []
    for k in range(X * ZH * C):
        x, zh, c = k // 4, k // 2 % 2, k % 2
        for s in range(N_SHARD):
            zl, y = divmod(s, Y)
            there = zl * C + c
            column = columns(zl)[(x, zh)] ^ (ZA * flip)
            pairs.append((k * N_SHARD + s, there * N_SHARD + column * Y + y))
    return pairs


def code_of(zl):
    return sum(p << 3 * (ZH * x + zh) for (x, zh), p in columns(zl).items())


class Slots:
    def __init__(self, here_ref):
        self.zb = here_ref[0] & 1
        self.core = here_ref[0] >> 1 & 1
        zl = here_ref[0] >> 2
        self.code = sum(jnp.where(zl == i, code_of(i), 0) for i in range(ZL))

    def halves(self):
        return (self.core, 1 - self.core)

    def home(self, j):
        return (self.code >> 3 * j) & 7

    def got(self, j):
        slot = self.home(j)
        return (slot & 3) * 2 + ((slot >> 2) ^ self.zb)


def homeward():
    return [(there, here) for here, there in outward()]


def dot(a, b, dims):
    return lax.dot_general(a, b, (dims, ((), ())), preferred_element_type=F32)


def as_column(row):
    n = row.shape[1]
    eye = lax.broadcasted_iota(jnp.int32, (n, n), 0) == lax.broadcasted_iota(jnp.int32, (n, n), 1)
    return jnp.sum(jnp.where(eye, jnp.broadcast_to(row, (n, n)), 0), axis=1, keepdims=True)


def pick_kernel(
    tok_hbm, cot_hbm, slot_hbm, gate_hbm, live_hbm, out_ref, tok, cot, slots, gates, live, sems
):
    moves = [
        pltpu.make_async_copy(source, target, sems.at[i])
        for i, (source, target) in enumerate(
            (
                (slot_hbm, slots),
                (gate_hbm, gates),
                (live_hbm, live),
                (tok_hbm, tok),
                (cot_hbm, cot),
            )
        )
    ]
    for move in moves:
        move.start()
    for move in moves:
        move.wait()
    spot = lax.broadcasted_iota(jnp.int32, (R, 64), 1)
    row = lax.broadcasted_iota(jnp.int32, (R, 1), 0)
    one_hot = [(as_column(slots[e : e + 1, :]) == spot).astype(BF16) for e in range(2)]
    scale = [jnp.where(row < live[e], as_column(gates[e : e + 1, :]), 0.0) for e in range(2)]
    for m, in_ref in enumerate((tok, cot)):
        values = in_ref[...]
        rows = [dot(one_hot[e], values, ((1,), (0,))) for e in range(2)]
        if m == 1:
            rows = [rows[e] * scale[e] for e in range(2)]
        out_ref[m * PACK : (m + 1) * PACK, :] = packed([part.astype(BF16) for part in rows])
    lane = lax.broadcasted_iota(jnp.int32, (8, 128), 1)
    line = lax.broadcasted_iota(jnp.int32, (8, 128), 0)
    note = jnp.where(lane == 0, live[0], 0) + jnp.where(lane == 64, live[1], 0)
    out_ref[2 * PACK :, :] = jnp.where(line == 0, note, 0).astype(F32).astype(BF16)


def packed(rows):
    left = jnp.concatenate([part[:, 128:] for part in rows], axis=1)
    return jnp.concatenate([part[:, :128] for part in rows] + [left], axis=0)


def features(at, slots, m, e):
    blocks = []
    for j in range(ZH * X):
        parts = []
        for h in range(2):
            block = at(h, slots.got(j))
            parts.append(block[m * PACK + e * R : m * PACK + (e + 1) * R, :])
            left = block[m * PACK + 2 * R : (m + 1) * PACK, :]
            parts.append(left[:, e * 64 : (e + 1) * 64])
        blocks.append(jnp.concatenate(parts, axis=1))
    return jnp.concatenate(blocks, axis=0)


def lines_of(got_ref, half):
    return lambda h, column: got_ref.at[2 * half + h, column]


def forward_kernel(
    dp_ref,
    got_ref,
    gate_ref,
    up_ref,
    gate_hbm,
    up_hbm,
    down_hbm,
    far_down_hbm,
    out_ref,
    far_gate,
    far_up,
    down_ref,
    far_down,
    sems,
):
    moves = [
        pltpu.make_async_copy(source, target, sems.at[i])
        for i, (source, target) in enumerate(
            (
                (gate_hbm, far_gate),
                (up_hbm, far_up),
                (down_hbm, down_ref),
                (far_down_hbm, far_down),
            )
        )
    ]
    for move in moves:
        move.start()
    slots = Slots(dp_ref)

    def give(t, e, part):
        out_ref[:, 2 * t + e] = part.astype(BF16).reshape(X, ZH * R, 512)

    def both(m, e):
        return [features(lines_of(got_ref, half), slots, m, e) for half in slots.halves()]

    rows = [both(0, e) for e in range(2)]
    inward = ((1,), (0,))
    near = [[dot(rows[e][0], ref[e], inward) for e in range(2)] for ref in (gate_ref, up_ref)]
    for t, ref in enumerate((far_gate, far_up)):
        moves[t].wait()
        for e in range(2):
            give(t, e, near[t][e] + dot(rows[e][1], ref[e], inward))
    moves[2].wait()
    moves[3].wait()
    for e in range(2):
        rows = both(1, e)
        across = ((1,), (1,))
        give(2, e, dot(rows[0], down_ref[e], across) + dot(rows[1], far_down[e], across))


def loan_kernel(dp_ref, got_ref, out_ref):
    slots = Slots(dp_ref)
    for h in range(2):
        out_ref[h] = got_ref[2 * (1 - slots.core) + h]


def spread_kernel(one_ref, two_ref, out_ref):
    for i in range(ZA):
        out_ref[i, 0] = one_ref[...]
        out_ref[i, 1] = two_ref[...]


def fold_kernel(in_ref, out_ref):
    total = sum(in_ref[i].astype(F32) for i in range(in_ref.shape[0]))
    out_ref[...] = total.astype(BF16)


def all_rows(refs, t, e):
    return jnp.concatenate([ref[:, 2 * t + e].reshape(ZH * X * R, 512) for ref in refs], axis=0)


def back_kernel(
    dp_ref, mine_ref, gate_ref, up_ref, gate_hbm, up_hbm, out_ref, far_gate, far_up, sems
):
    moves = [
        pltpu.make_async_copy(source, target, sems.at[i])
        for i, (source, target) in enumerate(((gate_hbm, far_gate), (up_hbm, far_up)))
    ]
    for move in moves:
        move.start()
    slots = Slots(dp_ref)
    grads = [[all_rows((mine_ref,), t, e) for t in (1, 2)] for e in range(2)]
    for half, weights in zip(slots.halves(), ((gate_ref, up_ref), (far_gate, far_up))):
        if weights[0] is far_gate:
            for move in moves:
                move.wait()
        terms = [
            sum(dot(grads[e][t], weights[t][e], ((1,), (1,))) for t in range(2)).astype(BF16)
            for e in range(2)
        ]
        for h in range(2):
            for j in range(ZH * X):
                rows = [term[j * R : (j + 1) * R, h * HALF : (h + 1) * HALF] for term in terms]
                out_ref[2 * half + h, slots.home(j)] = packed(rows)


def weight_kernel(dp_ref, got_ref, lent_ref, mine_ref, other_ref, gate_out, up_out, down_out):
    slots = Slots(dp_ref)
    notes = [ref[0, :, 2 * PACK :, :].astype(F32).reshape(ZL * 8, 128) for ref in (got_ref, lent_ref)]
    notes = jnp.concatenate(notes, axis=0)
    acts = (mine_ref, other_ref)
    for e in range(2):
        scale = 1.0 / jnp.full((1, 512), jnp.sum(notes[:, e * 64 : (e + 1) * 64]), F32)
        rows, cot = (
            jnp.concatenate(
                [
                    features(lines_of(got_ref, slots.core), slots, m, e),
                    features(lines_of(lent_ref, 0), slots, m, e),
                ],
                axis=0,
            )
            for m in range(2)
        )
        hidden, grad_gate, grad_up = (all_rows(acts, t, e) for t in range(3))
        gate_out[e] = (dot(rows, grad_gate, ((0,), (0,))) * scale).astype(BF16)
        up_out[e] = (dot(rows, grad_up, ((0,), (0,))) * scale).astype(BF16)
        down_out[e] = (dot(hidden, cot, ((0,), (0,))) * scale[:, :384]).astype(BF16)


def place_kernel(rows_ref, slot_ref, out_ref):
    spot = lax.broadcasted_iota(jnp.int32, (64, R), 0)
    total = jnp.zeros((64, HALF), F32)
    left = rows_ref[2 * R :, :]
    for e in range(2):
        one_hot = (spot == slot_ref[e : e + 1, :]).astype(BF16)
        rows = [rows_ref[e * R : (e + 1) * R, :], left[:, e * 64 : (e + 1) * 64]]
        total = total + dot(one_hot, jnp.concatenate(rows, axis=1), ((1,), (0,)))
    out_ref[...] = total.astype(BF16)


VM = pl.BlockSpec(memory_space=pltpu.VMEM)
SM = pl.BlockSpec(memory_space=pltpu.SMEM)
HB = pl.BlockSpec(memory_space=pltpu.HBM)


def in_vmem(x):
    return pltpu.with_memory_space_constraint(x, pltpu.VMEM)


def in_hbm(x):
    return pltpu.with_memory_space_constraint(x, pltpu.HBM)


def local(kernel, specs, outs, stay=True, scratch=()):
    if stay:
        shapes = [pltpu.VMEM(o, BF16) for o in outs]
    else:
        shapes = [pltpu.HBM(o, BF16) for o in outs]
    return pl.pallas_call(
        kernel,
        in_specs=specs,
        out_specs=[VM] * len(outs),
        out_shape=shapes,
        scratch_shapes=scratch,
        compiler_params=pltpu.CompilerParams(vmem_limit_bytes=16 << 20),
    )


def folded(tiles):
    (total,) = local(fold_kernel, [VM], [tiles.shape[1:]])(in_vmem(tiles))
    return total


def layer(
    tokens, cotangent, gate_proj, up_proj, down_proj, slot_tokens, gate_weights, live_counts
):
    dp = (lax.axis_index(DP) * ZB + lax.axis_index("zb")).astype(jnp.int32).reshape(1)
    scratch = [
        pltpu.VMEM(tokens.shape, BF16),
        pltpu.VMEM(cotangent.shape, BF16),
        pltpu.VMEM(slot_tokens.shape, jnp.int32),
        pltpu.VMEM(gate_weights.shape, F32),
        pltpu.SMEM((2,), jnp.int32),
        pltpu.SemaphoreType.DMA((5,)),
    ]
    (message,) = local(pick_kernel, [HB] * 5, [(MESSAGE, 128)], scratch=scratch)(
        *(
            in_hbm(a)
            for a in (tokens, cotangent, slot_tokens, gate_weights, live_counts.reshape(2))
        )
    )
    swap = [(0, 1), (1, 0)]
    messages = [lax.ppermute(message, EVERY, outward(flip)) for flip in range(2)]
    far = [lax.ppermute(w, "c", swap) for w in (gate_proj, up_proj, down_proj)]
    gate, up = in_vmem(gate_proj), in_vmem(up_proj)
    (copies,) = local(spread_kernel, [VM] * 2, [(ZA, ZB, MESSAGE, 128)], False)(*messages)
    column = lax.all_to_all(copies, "za", 0, 0, tiled=True).reshape(ZL, MESSAGE, 128)
    got = in_vmem(lax.all_gather(column, "y", axis=0, tiled=False))

    (parts,) = local(
        forward_kernel,
        [SM] + [VM] * 3 + [HB] * 4,
        [(X, 6, ZH * R, 512)],
        scratch=[pltpu.VMEM(gate.shape, BF16)] * 2
        + [pltpu.VMEM(down_proj.shape, BF16)] * 2
        + [pltpu.SemaphoreType.DMA((4,))],
    )(dp, got, gate, up, *(in_hbm(w) for w in (far[0], far[1], down_proj, far[2])))
    (loan,) = local(loan_kernel, [SM, VM], [(2, ZL, MESSAGE, 128)])(dp, got)
    lent = lax.ppermute(loan, "c", swap)
    over_x = lax.all_to_all(parts, "x", 0, 0, tiled=True)
    over_x = folded(over_x)
    over_zh = lax.all_gather(over_x, "zh", axis=0, tiled=False)
    sums = jnp.sum(over_zh.astype(F32), axis=0)
    gate_sum, up_sum, cot_hidden = sums[0:2], sums[2:4], sums[4:6]
    sigmoid_part = jax.nn.sigmoid(gate_sum)
    hidden = gate_sum * sigmoid_part * up_sum
    grad_gate = cot_hidden * up_sum * sigmoid_part * (1.0 + gate_sum * (1.0 - sigmoid_part))
    grad_up = cot_hidden * gate_sum * sigmoid_part
    acts = jnp.concatenate([hidden, grad_gate, grad_up], axis=0).astype(BF16)
    mine = lax.all_gather(acts, "x", axis=0, tiled=False)
    other = lax.ppermute(mine, "c", swap)
    mine = in_vmem(mine)

    (back,) = local(
        back_kernel,
        [SM] + [VM] * 3 + [HB] * 2,
        [(Y, ZL, PACK, 128)],
        False,
        [pltpu.VMEM(gate.shape, BF16)] * 2 + [pltpu.SemaphoreType.DMA((2,))],
    )(dp, mine, gate, up, in_hbm(far[0]), in_hbm(far[1]))
    over_y = lax.all_to_all(back, "y", 0, 0, tiled=True)
    over_y = folded(over_y)
    over_zl = lax.all_to_all(over_y, LINE, 0, 0, tiled=True)
    over_zl = jnp.sum(over_zl.astype(F32), axis=0).astype(BF16)
    home = lax.ppermute(over_zl, EVERY, homeward())
    home = in_vmem(home)
    grad_gate_proj, grad_up_proj, grad_down_proj = local(
        weight_kernel,
        [SM, VM, VM, VM, VM],
        [gate_proj.shape, up_proj.shape, down_proj.shape],
        False,
    )(dp, got, lent, mine, other)
    (grad_tokens,) = local(place_kernel, [VM, VM], [tokens.shape], False)(home, slot_tokens)
    return (grad_tokens, grad_gate_proj, grad_up_proj, grad_down_proj)


def solution(mesh):
    fine = Mesh(mesh.devices.reshape(X, ZH, C, ZB, ZA, Y), EVERY)
    in_specs = (
        P(DP, SHARD),
        P(DP, SHARD),
        P(None, DP, SHARD),
        P(None, DP, SHARD),
        P(None, SHARD, DP),
        P(None, DP),
        P(None, DP),
        P(None, DP),
    )
    out_specs = (
        P(DP, SHARD),
        P(None, DP, SHARD),
        P(None, DP, SHARD),
        P(None, SHARD, DP),
    )
    return jax.shard_map(layer, mesh=fine, in_specs=in_specs, out_specs=out_specs, check_vma=False)
```

```python
import jax
import jax.numpy as jnp
from jax import lax
from jax.experimental import pallas as pl
from jax.experimental.pallas import tpu as pltpu
from jax.sharding import Mesh, PartitionSpec as P

X, ZH, C, ZL, Y = 4, 2, 2, 8, 4
DP = ("x", "zh", "c")
SHARD = ("zl", "y")
EVERY = DP + SHARD
N_SHARD = ZL * Y
HALF = 192
R = 16
PACK = 3 * R
MESSAGE = 2 * PACK + 8
BF16 = jnp.bfloat16
F32 = jnp.float32


def ring(a, b, n):
    return min((a - b) % n, (b - a) % n)


def columns(zl):
    x_here, zh_here = divmod(zl, ZH)
    by_reach = sorted(range(ZL), key=lambda p: (abs(p - zl), p))
    by_ring = sorted(range(X), key=lambda x: (-ring(x, x_here, X), x))
    near = {(x, zh_here): p for x, p in zip(by_ring, by_reach[:4])}
    far = {(x, 1 - zh_here): p for x, p in zip(by_ring, by_reach[:3:-1])}
    return near | far


def outward():
    pairs = []
    for k in range(X * ZH * C):
        x, zh, c = k // 4, k // 2 % 2, k % 2
        for s in range(N_SHARD):
            zl, y = divmod(s, Y)
            there = zl * C + c
            column = columns(zl)[(x, zh)]
            pairs.append((k * N_SHARD + s, there * N_SHARD + column * Y + y))
    return pairs


def code_of(zl):
    return sum(p << 3 * (ZH * x + zh) for (x, zh), p in columns(zl).items())


class Slots:
    def __init__(self, dp_ref):
        self.core = dp_ref[0] & 1
        zl = dp_ref[0] >> 1
        self.code = sum(jnp.where(zl == i, code_of(i), 0) for i in range(ZL))

    def halves(self):
        return (self.core, 1 - self.core)

    def column(self, j):
        return (self.code >> 3 * j) & 7


def homeward():
    return [(there, here) for here, there in outward()]


def dot(a, b, dims):
    return lax.dot_general(a, b, (dims, ((), ())), preferred_element_type=F32)


def as_column(row):
    n = row.shape[1]
    eye = lax.broadcasted_iota(jnp.int32, (n, n), 0) == lax.broadcasted_iota(jnp.int32, (n, n), 1)
    return jnp.sum(jnp.where(eye, jnp.broadcast_to(row, (n, n)), 0), axis=1, keepdims=True)


def pick_kernel(
    tok_hbm, cot_hbm, slot_hbm, gate_hbm, live_hbm, out_ref, tok, cot, slots, gates, live, sems
):
    moves = [
        pltpu.make_async_copy(source, target, sems.at[i])
        for i, (source, target) in enumerate(
            (
                (slot_hbm, slots),
                (gate_hbm, gates),
                (live_hbm, live),
                (tok_hbm, tok),
                (cot_hbm, cot),
            )
        )
    ]
    for move in moves:
        move.start()
    for move in moves:
        move.wait()
    spot = lax.broadcasted_iota(jnp.int32, (R, 64), 1)
    row = lax.broadcasted_iota(jnp.int32, (R, 1), 0)
    one_hot = [(as_column(slots[e : e + 1, :]) == spot).astype(BF16) for e in range(2)]
    scale = [jnp.where(row < live[e], as_column(gates[e : e + 1, :]), 0.0) for e in range(2)]
    for m, in_ref in enumerate((tok, cot)):
        values = in_ref[...]
        rows = [dot(one_hot[e], values, ((1,), (0,))) for e in range(2)]
        if m == 1:
            rows = [rows[e] * scale[e] for e in range(2)]
        out_ref[m * PACK : (m + 1) * PACK, :] = packed([part.astype(BF16) for part in rows])
    lane = lax.broadcasted_iota(jnp.int32, (8, 128), 1)
    line = lax.broadcasted_iota(jnp.int32, (8, 128), 0)
    note = jnp.where(lane == 0, live[0], 0) + jnp.where(lane == 64, live[1], 0)
    out_ref[2 * PACK :, :] = jnp.where(line == 0, note, 0).astype(F32).astype(BF16)


def packed(rows):
    left = jnp.concatenate([part[:, 128:] for part in rows], axis=1)
    return jnp.concatenate([part[:, :128] for part in rows] + [left], axis=0)


def features(at, slots, m, e):
    blocks = []
    for j in range(ZH * X):
        parts = []
        for h in range(2):
            block = at(h, slots.column(j))
            parts.append(block[m * PACK + e * R : m * PACK + (e + 1) * R, :])
            left = block[m * PACK + 2 * R : (m + 1) * PACK, :]
            parts.append(left[:, e * 64 : (e + 1) * 64])
        blocks.append(jnp.concatenate(parts, axis=1))
    return jnp.concatenate(blocks, axis=0)


def lines_of(got_ref, half):
    return lambda h, column: got_ref.at[2 * half + h, column]


def forward_kernel(
    dp_ref,
    got_ref,
    gate_ref,
    up_ref,
    gate_hbm,
    up_hbm,
    down_hbm,
    far_down_hbm,
    out_ref,
    far_gate,
    far_up,
    down_ref,
    far_down,
    sems,
):
    moves = [
        pltpu.make_async_copy(source, target, sems.at[i])
        for i, (source, target) in enumerate(
            (
                (gate_hbm, far_gate),
                (up_hbm, far_up),
                (down_hbm, down_ref),
                (far_down_hbm, far_down),
            )
        )
    ]
    for move in moves:
        move.start()
    slots = Slots(dp_ref)

    def give(t, e, part):
        out_ref[:, 2 * t + e] = part.astype(BF16).reshape(X, ZH * R, 512)

    def both(m, e):
        return [features(lines_of(got_ref, half), slots, m, e) for half in slots.halves()]

    rows = [both(0, e) for e in range(2)]
    inward = ((1,), (0,))
    near = [[dot(rows[e][0], ref[e], inward) for e in range(2)] for ref in (gate_ref, up_ref)]
    for t, ref in enumerate((far_gate, far_up)):
        moves[t].wait()
        for e in range(2):
            give(t, e, near[t][e] + dot(rows[e][1], ref[e], inward))
    moves[2].wait()
    moves[3].wait()
    for e in range(2):
        rows = both(1, e)
        across = ((1,), (1,))
        give(2, e, dot(rows[0], down_ref[e], across) + dot(rows[1], far_down[e], across))


def loan_kernel(dp_ref, got_ref, out_ref):
    slots = Slots(dp_ref)
    for h in range(2):
        out_ref[h] = got_ref[2 * (1 - slots.core) + h]


def fold_kernel(in_ref, out_ref):
    total = sum(in_ref[i].astype(F32) for i in range(in_ref.shape[0]))
    out_ref[...] = total.astype(BF16)


def all_rows(refs, t, e):
    return jnp.concatenate([ref[:, 2 * t + e].reshape(ZH * X * R, 512) for ref in refs], axis=0)


def back_kernel(dp_ref, mine_ref, gate_ref, up_ref, far_gate, far_up, out_ref):
    slots = Slots(dp_ref)
    grads = [[all_rows((mine_ref,), t, e) for t in (1, 2)] for e in range(2)]
    for half, weights in zip(slots.halves(), ((gate_ref, up_ref), (far_gate, far_up))):
        terms = [
            sum(dot(grads[e][t], weights[t][e], ((1,), (1,))) for t in range(2)).astype(BF16)
            for e in range(2)
        ]
        for h in range(2):
            for j in range(ZH * X):
                rows = [term[j * R : (j + 1) * R, h * HALF : (h + 1) * HALF] for term in terms]
                out_ref[2 * half + h, slots.column(j)] = packed(rows)


def weight_kernel(dp_ref, got_ref, lent_ref, mine_ref, other_ref, gate_out, up_out, down_out):
    slots = Slots(dp_ref)
    notes = [ref[0, :, 2 * PACK :, :].astype(F32).reshape(ZL * 8, 128) for ref in (got_ref, lent_ref)]
    notes = jnp.concatenate(notes, axis=0)
    acts = (mine_ref, other_ref)
    for e in range(2):
        scale = 1.0 / jnp.full((1, 512), jnp.sum(notes[:, e * 64 : (e + 1) * 64]), F32)
        rows, cot = (
            jnp.concatenate(
                [
                    features(lines_of(got_ref, slots.core), slots, m, e),
                    features(lines_of(lent_ref, 0), slots, m, e),
                ],
                axis=0,
            )
            for m in range(2)
        )
        hidden, grad_gate, grad_up = (all_rows(acts, t, e) for t in range(3))
        gate_out[e] = (dot(rows, grad_gate, ((0,), (0,))) * scale).astype(BF16)
        up_out[e] = (dot(rows, grad_up, ((0,), (0,))) * scale).astype(BF16)
        down_out[e] = (dot(hidden, cot, ((0,), (0,))) * scale[:, :384]).astype(BF16)


def place_kernel(rows_ref, slot_ref, out_ref):
    spot = lax.broadcasted_iota(jnp.int32, (64, R), 0)
    total = jnp.zeros((64, HALF), F32)
    left = rows_ref[2 * R :, :]
    for e in range(2):
        one_hot = (spot == slot_ref[e : e + 1, :]).astype(BF16)
        rows = [rows_ref[e * R : (e + 1) * R, :], left[:, e * 64 : (e + 1) * 64]]
        total = total + dot(one_hot, jnp.concatenate(rows, axis=1), ((1,), (0,)))
    out_ref[...] = total.astype(BF16)


VM = pl.BlockSpec(memory_space=pltpu.VMEM)
SM = pl.BlockSpec(memory_space=pltpu.SMEM)
HB = pl.BlockSpec(memory_space=pltpu.HBM)


def in_vmem(x):
    return pltpu.with_memory_space_constraint(x, pltpu.VMEM)


def in_hbm(x):
    return pltpu.with_memory_space_constraint(x, pltpu.HBM)


def local(kernel, specs, outs, stay=True, scratch=()):
    if stay:
        shapes = [pltpu.VMEM(o, BF16) for o in outs]
    else:
        shapes = [pltpu.HBM(o, BF16) for o in outs]
    return pl.pallas_call(
        kernel,
        in_specs=specs,
        out_specs=[VM] * len(outs),
        out_shape=shapes,
        scratch_shapes=scratch,
        compiler_params=pltpu.CompilerParams(vmem_limit_bytes=16 << 20),
    )


def folded(tiles, stay=True):
    (total,) = local(fold_kernel, [VM], [tiles.shape[1:]], stay)(in_vmem(tiles))
    return total


def layer(
    tokens, cotangent, gate_proj, up_proj, down_proj, slot_tokens, gate_weights, live_counts
):
    dp = lax.axis_index(DP).astype(jnp.int32).reshape(1)
    scratch = [
        pltpu.VMEM(tokens.shape, BF16),
        pltpu.VMEM(cotangent.shape, BF16),
        pltpu.VMEM(slot_tokens.shape, jnp.int32),
        pltpu.VMEM(gate_weights.shape, F32),
        pltpu.SMEM((2,), jnp.int32),
        pltpu.SemaphoreType.DMA((5,)),
    ]
    (message,) = local(pick_kernel, [HB] * 5, [(MESSAGE, 128)], scratch=scratch)(
        *(
            in_hbm(a)
            for a in (tokens, cotangent, slot_tokens, gate_weights, live_counts.reshape(2))
        )
    )
    swap = [(0, 1), (1, 0)]
    message = lax.ppermute(message, EVERY, outward())
    far = [lax.ppermute(w, "c", swap) for w in (gate_proj, up_proj, down_proj)]
    gate, up = in_vmem(gate_proj), in_vmem(up_proj)
    copies = jnp.broadcast_to(message[None], (ZL, MESSAGE, 128))
    column = lax.all_to_all(copies, "zl", 0, 0, tiled=True)
    got = in_vmem(lax.all_gather(column, "y", axis=0, tiled=False))

    parts, far_gate, far_up = local(
        forward_kernel,
        [SM] + [VM] * 3 + [HB] * 4,
        [(X, 6, ZH * R, 512), gate.shape, up.shape],
        scratch=[pltpu.VMEM(down_proj.shape, BF16)] * 2 + [pltpu.SemaphoreType.DMA((4,))],
    )(dp, got, gate, up, *(in_hbm(w) for w in (far[0], far[1], down_proj, far[2])))
    (loan,) = local(loan_kernel, [SM, VM], [(2, ZL, MESSAGE, 128)])(dp, got)
    lent = lax.ppermute(loan, "c", swap)
    over_x = lax.all_to_all(parts, "x", 0, 0, tiled=True)
    over_x = folded(over_x)
    over_zh = lax.all_gather(over_x, "zh", axis=0, tiled=False)
    sums = jnp.sum(over_zh.astype(F32), axis=0)
    gate_sum, up_sum, cot_hidden = sums[0:2], sums[2:4], sums[4:6]
    sigmoid_part = jax.nn.sigmoid(gate_sum)
    hidden = gate_sum * sigmoid_part * up_sum
    grad_gate = cot_hidden * up_sum * sigmoid_part * (1.0 + gate_sum * (1.0 - sigmoid_part))
    grad_up = cot_hidden * gate_sum * sigmoid_part
    acts = jnp.concatenate([hidden, grad_gate, grad_up], axis=0).astype(BF16)
    mine = lax.all_gather(acts, "x", axis=0, tiled=False)
    other = lax.ppermute(mine, "c", swap)
    mine = in_vmem(mine)

    (back,) = local(back_kernel, [SM] + [VM] * 5, [(Y, ZL, PACK, 128)], False)(
        dp, mine, gate, up, far_gate, far_up
    )
    over_y = lax.all_to_all(back, "y", 0, 0, tiled=True)
    over_y = folded(over_y, False)
    over_zl = lax.all_to_all(over_y, "zl", 0, 0, tiled=True)
    over_zl = jnp.sum(over_zl.astype(F32), axis=0).astype(BF16)
    home = lax.ppermute(over_zl, EVERY, homeward())
    home = in_vmem(home)
    grad_gate_proj, grad_up_proj, grad_down_proj = local(
        weight_kernel,
        [SM, VM, VM, VM, VM],
        [gate_proj.shape, up_proj.shape, down_proj.shape],
        False,
    )(dp, got, lent, mine, other)
    (grad_tokens,) = local(place_kernel, [VM, VM], [tokens.shape], False)(home, slot_tokens)
    return (grad_tokens, grad_gate_proj, grad_up_proj, grad_down_proj)


def solution(mesh):
    fine = Mesh(mesh.devices.reshape(X, ZH, C, ZL, Y), EVERY)
    in_specs = (
        P(DP, SHARD),
        P(DP, SHARD),
        P(None, DP, SHARD),
        P(None, DP, SHARD),
        P(None, SHARD, DP),
        P(None, DP),
        P(None, DP),
        P(None, DP),
    )
    out_specs = (
        P(DP, SHARD),
        P(None, DP, SHARD),
        P(None, DP, SHARD),
        P(None, SHARD, DP),
    )
    return jax.shard_map(layer, mesh=fine, in_specs=in_specs, out_specs=out_specs, check_vma=False)
```

```python
import jax
import jax.numpy as jnp
from jax import lax
from jax.experimental import pallas as pl
from jax.experimental.pallas import tpu as pltpu
from jax.sharding import Mesh, PartitionSpec as P

X, ZH, C, ZL, Y = 4, 2, 2, 8, 4
DP = ("x", "zh", "c")
SHARD = ("zl", "y")
EVERY = DP + SHARD
N_SHARD = ZL * Y
HALF = 192
R = 16
PACK = 3 * R
MESSAGE = 2 * PACK + 8
BF16 = jnp.bfloat16
F32 = jnp.float32


def ring(a, b, n):
    return min((a - b) % n, (b - a) % n)


def columns(zl):
    x_here, zh_here = divmod(zl, ZH)
    by_reach = sorted(range(ZL), key=lambda p: (abs(p - zl), p))
    by_ring = sorted(range(X), key=lambda x: (-ring(x, x_here, X), x))
    near = {(x, zh_here): p for x, p in zip(by_ring, by_reach[:4])}
    far = {(x, 1 - zh_here): p for x, p in zip(by_ring, by_reach[:3:-1])}
    return near | far


def outward():
    pairs = []
    for k in range(X * ZH * C):
        x, zh, c = k // 4, k // 2 % 2, k % 2
        for s in range(N_SHARD):
            zl, y = divmod(s, Y)
            there = zl * C + c
            column = columns(zl)[(x, zh)]
            pairs.append((k * N_SHARD + s, there * N_SHARD + column * Y + y))
    return pairs


def code_of(zl):
    return sum(p << 3 * (ZH * x + zh) for (x, zh), p in columns(zl).items())


class Slots:
    def __init__(self, dp_ref):
        self.core = dp_ref[0] & 1
        zl = dp_ref[0] >> 1
        self.code = sum(jnp.where(zl == i, code_of(i), 0) for i in range(ZL))

    def halves(self):
        return (self.core, 1 - self.core)

    def column(self, j):
        return (self.code >> 3 * j) & 7


def homeward():
    return [(there, here) for here, there in outward()]


def dot(a, b, dims):
    return lax.dot_general(a, b, (dims, ((), ())), preferred_element_type=F32)


def as_column(row):
    n = row.shape[1]
    eye = lax.broadcasted_iota(jnp.int32, (n, n), 0) == lax.broadcasted_iota(jnp.int32, (n, n), 1)
    return jnp.sum(jnp.where(eye, jnp.broadcast_to(row, (n, n)), 0), axis=1, keepdims=True)


def pick_kernel(
    tok_hbm, cot_hbm, slot_hbm, gate_hbm, live_hbm, out_ref, tok, cot, slots, gates, live, sems
):
    moves = [
        pltpu.make_async_copy(source, target, sems.at[i])
        for i, (source, target) in enumerate(
            (
                (slot_hbm, slots),
                (gate_hbm, gates),
                (live_hbm, live),
                (tok_hbm, tok),
                (cot_hbm, cot),
            )
        )
    ]
    for move in moves:
        move.start()
    for move in moves:
        move.wait()
    spot = lax.broadcasted_iota(jnp.int32, (R, 64), 1)
    row = lax.broadcasted_iota(jnp.int32, (R, 1), 0)
    one_hot = [(as_column(slots[e : e + 1, :]) == spot).astype(BF16) for e in range(2)]
    scale = [jnp.where(row < live[e], as_column(gates[e : e + 1, :]), 0.0) for e in range(2)]
    for m, in_ref in enumerate((tok, cot)):
        values = in_ref[...]
        rows = [dot(one_hot[e], values, ((1,), (0,))) for e in range(2)]
        if m == 1:
            rows = [rows[e] * scale[e] for e in range(2)]
        out_ref[m * PACK : (m + 1) * PACK, :] = packed([part.astype(BF16) for part in rows])
    lane = lax.broadcasted_iota(jnp.int32, (8, 128), 1)
    line = lax.broadcasted_iota(jnp.int32, (8, 128), 0)
    note = jnp.where(lane == 0, live[0], 0) + jnp.where(lane == 64, live[1], 0)
    out_ref[2 * PACK :, :] = jnp.where(line == 0, note, 0).astype(F32).astype(BF16)


def packed(rows):
    left = jnp.concatenate([part[:, 128:] for part in rows], axis=1)
    return jnp.concatenate([part[:, :128] for part in rows] + [left], axis=0)


def features(at, slots, m, e):
    blocks = []
    for j in range(ZH * X):
        parts = []
        for h in range(2):
            block = at(h, slots.column(j))
            parts.append(block[m * PACK + e * R : m * PACK + (e + 1) * R, :])
            left = block[m * PACK + 2 * R : (m + 1) * PACK, :]
            parts.append(left[:, e * 64 : (e + 1) * 64])
        blocks.append(jnp.concatenate(parts, axis=1))
    return jnp.concatenate(blocks, axis=0)


def lines_of(got_ref, half):
    return lambda h, column: got_ref.at[2 * half + h, column]


def forward_kernel(
    dp_ref, got_ref, gate_ref, far_gate, up_ref, up_hbm, down_hbm, far_hbm, out_ref, *scratch
):
    far_up, down_ref, far_down, sems = scratch
    moves = [
        pltpu.make_async_copy(source, target, sems.at[i])
        for i, (source, target) in enumerate(
            ((up_hbm, far_up), (down_hbm, down_ref), (far_hbm, far_down))
        )
    ]
    for move in moves:
        move.start()
    slots = Slots(dp_ref)

    def give(t, e, rows, pair, dims):
        part = dot(rows[0], pair[0][e], dims) + dot(rows[1], pair[1][e], dims)
        out_ref[:, 2 * t + e] = part.astype(BF16).reshape(X, ZH * R, 512)

    def both(m, e):
        return [features(lines_of(got_ref, half), slots, m, e) for half in slots.halves()]

    rows = [both(0, e) for e in range(2)]
    for e in range(2):
        give(0, e, rows[e], (gate_ref, far_gate), ((1,), (0,)))
    moves[0].wait()
    for e in range(2):
        give(1, e, rows[e], (up_ref, far_up), ((1,), (0,)))
    moves[1].wait()
    moves[2].wait()
    for e in range(2):
        give(2, e, both(1, e), (down_ref, far_down), ((1,), (1,)))


def loan_kernel(dp_ref, got_ref, out_ref):
    slots = Slots(dp_ref)
    for h in range(2):
        out_ref[h] = got_ref[2 * (1 - slots.core) + h]


def fold_kernel(in_ref, out_ref):
    total = sum(in_ref[i].astype(F32) for i in range(in_ref.shape[0]))
    out_ref[...] = total.astype(BF16)


def all_rows(refs, t, e):
    return jnp.concatenate([ref[:, 2 * t + e].reshape(ZH * X * R, 512) for ref in refs], axis=0)


def back_kernel(
    dp_ref, mine_ref, gate_ref, far_gate, up_ref, up_hbm, out_ref, far_up, sem
):
    move = pltpu.make_async_copy(up_hbm, far_up, sem)
    move.start()
    slots = Slots(dp_ref)
    grads = [[all_rows((mine_ref,), t, e) for t in (1, 2)] for e in range(2)]
    for half, weights in zip(slots.halves(), ((gate_ref, up_ref), (far_gate, far_up))):
        if weights[1] is far_up:
            move.wait()
        terms = [
            sum(dot(grads[e][t], weights[t][e], ((1,), (1,))) for t in range(2)).astype(BF16)
            for e in range(2)
        ]
        for h in range(2):
            for j in range(ZH * X):
                rows = [term[j * R : (j + 1) * R, h * HALF : (h + 1) * HALF] for term in terms]
                out_ref[2 * half + h, slots.column(j)] = packed(rows)


def weight_kernel(dp_ref, got_ref, lent_ref, mine_ref, other_ref, gate_out, up_out, down_out):
    slots = Slots(dp_ref)
    notes = [ref[0, :, 2 * PACK :, :].astype(F32).reshape(ZL * 8, 128) for ref in (got_ref, lent_ref)]
    notes = jnp.concatenate(notes, axis=0)
    acts = (mine_ref, other_ref)
    for e in range(2):
        scale = 1.0 / jnp.full((1, 512), jnp.sum(notes[:, e * 64 : (e + 1) * 64]), F32)
        rows, cot = (
            jnp.concatenate(
                [
                    features(lines_of(got_ref, slots.core), slots, m, e),
                    features(lines_of(lent_ref, 0), slots, m, e),
                ],
                axis=0,
            )
            for m in range(2)
        )
        hidden, grad_gate, grad_up = (all_rows(acts, t, e) for t in range(3))
        gate_out[e] = (dot(rows, grad_gate, ((0,), (0,))) * scale).astype(BF16)
        up_out[e] = (dot(rows, grad_up, ((0,), (0,))) * scale).astype(BF16)
        down_out[e] = (dot(hidden, cot, ((0,), (0,))) * scale[:, :384]).astype(BF16)


def place_kernel(rows_ref, slot_ref, out_ref):
    spot = lax.broadcasted_iota(jnp.int32, (64, R), 0)
    total = jnp.zeros((64, HALF), F32)
    left = rows_ref[2 * R :, :]
    for e in range(2):
        one_hot = (spot == slot_ref[e : e + 1, :]).astype(BF16)
        rows = [rows_ref[e * R : (e + 1) * R, :], left[:, e * 64 : (e + 1) * 64]]
        total = total + dot(one_hot, jnp.concatenate(rows, axis=1), ((1,), (0,)))
    out_ref[...] = total.astype(BF16)


VM = pl.BlockSpec(memory_space=pltpu.VMEM)
SM = pl.BlockSpec(memory_space=pltpu.SMEM)
HB = pl.BlockSpec(memory_space=pltpu.HBM)


def in_vmem(x):
    return pltpu.with_memory_space_constraint(x, pltpu.VMEM)


def in_hbm(x):
    return pltpu.with_memory_space_constraint(x, pltpu.HBM)


def local(kernel, specs, outs, stay=True, scratch=()):
    if stay:
        shapes = [pltpu.VMEM(o, BF16) for o in outs]
    else:
        shapes = [pltpu.HBM(o, BF16) for o in outs]
    return pl.pallas_call(
        kernel,
        in_specs=specs,
        out_specs=[VM] * len(outs),
        out_shape=shapes,
        scratch_shapes=scratch,
        compiler_params=pltpu.CompilerParams(vmem_limit_bytes=16 << 20),
    )


def folded(tiles, stay=True):
    (total,) = local(fold_kernel, [VM], [tiles.shape[1:]], stay)(in_vmem(tiles))
    return total


def layer(
    tokens, cotangent, gate_proj, up_proj, down_proj, slot_tokens, gate_weights, live_counts
):
    dp = lax.axis_index(DP).astype(jnp.int32).reshape(1)
    scratch = [
        pltpu.VMEM(tokens.shape, BF16),
        pltpu.VMEM(cotangent.shape, BF16),
        pltpu.VMEM(slot_tokens.shape, jnp.int32),
        pltpu.VMEM(gate_weights.shape, F32),
        pltpu.SMEM((2,), jnp.int32),
        pltpu.SemaphoreType.DMA((5,)),
    ]
    (message,) = local(pick_kernel, [HB] * 5, [(MESSAGE, 128)], scratch=scratch)(
        *(
            in_hbm(a)
            for a in (tokens, cotangent, slot_tokens, gate_weights, live_counts.reshape(2))
        )
    )
    swap = [(0, 1), (1, 0)]
    message = lax.ppermute(message, EVERY, outward())
    far = [lax.ppermute(w, "c", swap) for w in (gate_proj, up_proj, down_proj)]
    held = [in_vmem(w) for w in (gate_proj, far[0], up_proj)] + [in_hbm(far[1])]
    copies = jnp.broadcast_to(message[None], (ZL, MESSAGE, 128))
    column = lax.all_to_all(copies, "zl", 0, 0, tiled=True)
    got = in_vmem(lax.all_gather(column, "y", axis=0, tiled=False))

    (parts,) = local(
        forward_kernel,
        [SM] + [VM] * 4 + [HB] * 3,
        [(X, 6, ZH * R, 512)],
        scratch=[pltpu.VMEM(w.shape, BF16) for w in (up_proj, down_proj, down_proj)]
        + [pltpu.SemaphoreType.DMA((3,))],
    )(dp, got, *held, in_hbm(down_proj), in_hbm(far[2]))
    (loan,) = local(loan_kernel, [SM, VM], [(2, ZL, MESSAGE, 128)])(dp, got)
    lent = lax.ppermute(loan, "c", swap)
    over_x = lax.all_to_all(parts, "x", 0, 0, tiled=True)
    over_x = folded(over_x)
    over_zh = lax.all_gather(over_x, "zh", axis=0, tiled=False)
    sums = jnp.sum(over_zh.astype(F32), axis=0)
    gate_sum, up_sum, cot_hidden = sums[0:2], sums[2:4], sums[4:6]
    sigmoid_part = jax.nn.sigmoid(gate_sum)
    hidden = gate_sum * sigmoid_part * up_sum
    grad_gate = cot_hidden * up_sum * sigmoid_part * (1.0 + gate_sum * (1.0 - sigmoid_part))
    grad_up = cot_hidden * gate_sum * sigmoid_part
    acts = jnp.concatenate([hidden, grad_gate, grad_up], axis=0).astype(BF16)
    mine = lax.all_gather(acts, "x", axis=0, tiled=False)
    other = lax.ppermute(mine, "c", swap)
    mine = in_vmem(mine)

    (back,) = local(
        back_kernel,
        [SM] + [VM] * 4 + [HB],
        [(Y, ZL, PACK, 128)],
        scratch=[pltpu.VMEM(up_proj.shape, BF16), pltpu.SemaphoreType.DMA],
    )(dp, mine, *held)
    over_y = lax.all_to_all(back, "y", 0, 0, tiled=True)
    over_y = folded(over_y, False)
    over_zl = lax.all_to_all(over_y, "zl", 0, 0, tiled=True)
    over_zl = jnp.sum(over_zl.astype(F32), axis=0).astype(BF16)
    home = lax.ppermute(over_zl, EVERY, homeward())
    home = in_vmem(home)
    grad_gate_proj, grad_up_proj, grad_down_proj = local(
        weight_kernel,
        [SM, VM, VM, VM, VM],
        [gate_proj.shape, up_proj.shape, down_proj.shape],
        False,
    )(dp, got, lent, mine, other)
    (grad_tokens,) = local(place_kernel, [VM, VM], [tokens.shape], False)(home, slot_tokens)
    return (grad_tokens, grad_gate_proj, grad_up_proj, grad_down_proj)


def solution(mesh):
    fine = Mesh(mesh.devices.reshape(X, ZH, C, ZL, Y), EVERY)
    in_specs = (
        P(DP, SHARD),
        P(DP, SHARD),
        P(None, DP, SHARD),
        P(None, DP, SHARD),
        P(None, SHARD, DP),
        P(None, DP),
        P(None, DP),
        P(None, DP),
    )
    out_specs = (
        P(DP, SHARD),
        P(None, DP, SHARD),
        P(None, DP, SHARD),
        P(None, SHARD, DP),
    )
    return jax.shard_map(layer, mesh=fine, in_specs=in_specs, out_specs=out_specs, check_vma=False)
```

```python
import jax
import jax.numpy as jnp
from jax import lax
from jax.experimental import pallas as pl
from jax.experimental.pallas import tpu as pltpu
from jax.sharding import Mesh, PartitionSpec as P

X, ZH, C, ZL, Y = 4, 2, 2, 8, 4
DP = ("x", "zh", "c")
SHARD = ("zl", "y")
EVERY = DP + SHARD
N_SHARD = ZL * Y
HALF = 192
R = 16
PACK = 3 * R
MESSAGE = 2 * PACK + 8
BF16 = jnp.bfloat16
F32 = jnp.float32


def ring(a, b, n):
    return min((a - b) % n, (b - a) % n)


def columns(zl):
    x_here, zh_here = divmod(zl, ZH)
    by_reach = sorted(range(ZL), key=lambda p: (abs(p - zl), p))
    by_ring = sorted(range(X), key=lambda x: (-ring(x, x_here, X), x))
    near = {(x, zh_here): p for x, p in zip(by_ring, by_reach[:4])}
    far = {(x, 1 - zh_here): p for x, p in zip(by_ring, by_reach[:3:-1])}
    return near | far


def outward():
    pairs = []
    for k in range(X * ZH * C):
        x, zh, c = k // 4, k // 2 % 2, k % 2
        for s in range(N_SHARD):
            zl, y = divmod(s, Y)
            there = zl * C + c
            column = columns(zl)[(x, zh)]
            pairs.append((k * N_SHARD + s, there * N_SHARD + column * Y + y))
    return pairs


def code_of(zl):
    return sum(p << 3 * (ZH * x + zh) for (x, zh), p in columns(zl).items())


class Slots:
    def __init__(self, dp_ref):
        self.core = dp_ref[0] & 1
        zl = dp_ref[0] >> 1
        self.code = sum(jnp.where(zl == i, code_of(i), 0) for i in range(ZL))

    def halves(self):
        return (self.core, 1 - self.core)

    def column(self, j):
        return (self.code >> 3 * j) & 7


def homeward():
    return [(there, here) for here, there in outward()]


def dot(a, b, dims):
    return lax.dot_general(a, b, (dims, ((), ())), preferred_element_type=F32)


def as_column(row):
    n = row.shape[1]
    eye = lax.broadcasted_iota(jnp.int32, (n, n), 0) == lax.broadcasted_iota(jnp.int32, (n, n), 1)
    return jnp.sum(jnp.where(eye, jnp.broadcast_to(row, (n, n)), 0), axis=1, keepdims=True)


def pick_kernel(
    tok_hbm, cot_hbm, slot_hbm, gate_hbm, live_hbm, out_ref, tok, cot, slots, gates, live, sems
):
    moves = [
        pltpu.make_async_copy(source, target, sems.at[i])
        for i, (source, target) in enumerate(
            (
                (slot_hbm, slots),
                (gate_hbm, gates),
                (live_hbm, live),
                (tok_hbm, tok),
                (cot_hbm, cot),
            )
        )
    ]
    for move in moves:
        move.start()
    for move in moves:
        move.wait()
    spot = lax.broadcasted_iota(jnp.int32, (R, 64), 1)
    row = lax.broadcasted_iota(jnp.int32, (R, 1), 0)
    one_hot = [(as_column(slots[e : e + 1, :]) == spot).astype(BF16) for e in range(2)]
    scale = [jnp.where(row < live[e], as_column(gates[e : e + 1, :]), 0.0) for e in range(2)]
    for m, in_ref in enumerate((tok, cot)):
        values = in_ref[...]
        rows = [dot(one_hot[e], values, ((1,), (0,))) for e in range(2)]
        if m == 1:
            rows = [rows[e] * scale[e] for e in range(2)]
        out_ref[m * PACK : (m + 1) * PACK, :] = packed([part.astype(BF16) for part in rows])
    lane = lax.broadcasted_iota(jnp.int32, (8, 128), 1)
    line = lax.broadcasted_iota(jnp.int32, (8, 128), 0)
    note = jnp.where(lane == 0, live[0], 0) + jnp.where(lane == 64, live[1], 0)
    out_ref[2 * PACK :, :] = jnp.where(line == 0, note, 0).astype(F32).astype(BF16)


def packed(rows):
    left = jnp.concatenate([part[:, 128:] for part in rows], axis=1)
    return jnp.concatenate([part[:, :128] for part in rows] + [left], axis=0)


def features(at, slots, m, e):
    blocks = []
    for j in range(ZH * X):
        parts = []
        for h in range(2):
            block = at(h, slots.column(j))
            parts.append(block[m * PACK + e * R : m * PACK + (e + 1) * R, :])
            left = block[m * PACK + 2 * R : (m + 1) * PACK, :]
            parts.append(left[:, e * 64 : (e + 1) * 64])
        blocks.append(jnp.concatenate(parts, axis=1))
    return jnp.concatenate(blocks, axis=0)


def lines_of(got_ref, half):
    return lambda h, column: got_ref.at[2 * half + h, column]


def forward_kernel(
    dp_ref, got_ref, gate_ref, far_gate, up_ref, up_hbm, down_hbm, far_hbm, out_ref, far_up, *scratch
):
    down_ref, far_down, sems = scratch
    moves = [
        pltpu.make_async_copy(source, target, sems.at[i])
        for i, (source, target) in enumerate(
            ((up_hbm, far_up), (down_hbm, down_ref), (far_hbm, far_down))
        )
    ]
    for move in moves:
        move.start()
    slots = Slots(dp_ref)

    def give(t, e, rows, pair, dims):
        part = dot(rows[0], pair[0][e], dims) + dot(rows[1], pair[1][e], dims)
        out_ref[:, 2 * t + e] = part.astype(BF16).reshape(X, ZH * R, 512)

    def both(m, e):
        return [features(lines_of(got_ref, half), slots, m, e) for half in slots.halves()]

    rows = [both(0, e) for e in range(2)]
    for e in range(2):
        give(0, e, rows[e], (gate_ref, far_gate), ((1,), (0,)))
    moves[0].wait()
    for e in range(2):
        give(1, e, rows[e], (up_ref, far_up), ((1,), (0,)))
    moves[1].wait()
    moves[2].wait()
    for e in range(2):
        give(2, e, both(1, e), (down_ref, far_down), ((1,), (1,)))


def loan_kernel(dp_ref, got_ref, out_ref):
    slots = Slots(dp_ref)
    for h in range(2):
        out_ref[h] = got_ref[2 * (1 - slots.core) + h]


def fold_kernel(in_ref, out_ref):
    total = sum(in_ref[i].astype(F32) for i in range(in_ref.shape[0]))
    out_ref[...] = total.astype(BF16)


def all_rows(refs, t, e):
    return jnp.concatenate([ref[:, 2 * t + e].reshape(ZH * X * R, 512) for ref in refs], axis=0)


def back_kernel(dp_ref, mine_ref, gate_ref, far_gate, up_ref, far_up, out_ref):
    slots = Slots(dp_ref)
    grads = [[all_rows((mine_ref,), t, e) for t in (1, 2)] for e in range(2)]
    for half, weights in zip(slots.halves(), ((gate_ref, up_ref), (far_gate, far_up))):
        terms = [
            sum(dot(grads[e][t], weights[t][e], ((1,), (1,))) for t in range(2)).astype(BF16)
            for e in range(2)
        ]
        for h in range(2):
            for j in range(ZH * X):
                rows = [term[j * R : (j + 1) * R, h * HALF : (h + 1) * HALF] for term in terms]
                out_ref[2 * half + h, slots.column(j)] = packed(rows)


def weight_kernel(dp_ref, got_ref, lent_ref, mine_ref, other_ref, gate_out, up_out, down_out):
    slots = Slots(dp_ref)
    notes = [ref[0, :, 2 * PACK :, :].astype(F32).reshape(ZL * 8, 128) for ref in (got_ref, lent_ref)]
    notes = jnp.concatenate(notes, axis=0)
    acts = (mine_ref, other_ref)
    for e in range(2):
        scale = 1.0 / jnp.full((1, 512), jnp.sum(notes[:, e * 64 : (e + 1) * 64]), F32)
        rows, cot = (
            jnp.concatenate(
                [
                    features(lines_of(got_ref, slots.core), slots, m, e),
                    features(lines_of(lent_ref, 0), slots, m, e),
                ],
                axis=0,
            )
            for m in range(2)
        )
        hidden, grad_gate, grad_up = (all_rows(acts, t, e) for t in range(3))
        gate_out[e] = (dot(rows, grad_gate, ((0,), (0,))) * scale).astype(BF16)
        up_out[e] = (dot(rows, grad_up, ((0,), (0,))) * scale).astype(BF16)
        down_out[e] = (dot(hidden, cot, ((0,), (0,))) * scale[:, :384]).astype(BF16)


def place_kernel(rows_ref, slot_ref, out_ref):
    spot = lax.broadcasted_iota(jnp.int32, (64, R), 0)
    total = jnp.zeros((64, HALF), F32)
    left = rows_ref[2 * R :, :]
    for e in range(2):
        one_hot = (spot == slot_ref[e : e + 1, :]).astype(BF16)
        rows = [rows_ref[e * R : (e + 1) * R, :], left[:, e * 64 : (e + 1) * 64]]
        total = total + dot(one_hot, jnp.concatenate(rows, axis=1), ((1,), (0,)))
    out_ref[...] = total.astype(BF16)


VM = pl.BlockSpec(memory_space=pltpu.VMEM)
SM = pl.BlockSpec(memory_space=pltpu.SMEM)
HB = pl.BlockSpec(memory_space=pltpu.HBM)


def in_vmem(x):
    return pltpu.with_memory_space_constraint(x, pltpu.VMEM)


def in_hbm(x):
    return pltpu.with_memory_space_constraint(x, pltpu.HBM)


def local(kernel, specs, outs, stay=True, scratch=()):
    if stay:
        shapes = [pltpu.VMEM(o, BF16) for o in outs]
    else:
        shapes = [pltpu.HBM(o, BF16) for o in outs]
    return pl.pallas_call(
        kernel,
        in_specs=specs,
        out_specs=[VM] * len(outs),
        out_shape=shapes,
        scratch_shapes=scratch,
        compiler_params=pltpu.CompilerParams(vmem_limit_bytes=16 << 20),
    )


def folded(tiles, stay=True):
    (total,) = local(fold_kernel, [VM], [tiles.shape[1:]], stay)(in_vmem(tiles))
    return total


def layer(
    tokens, cotangent, gate_proj, up_proj, down_proj, slot_tokens, gate_weights, live_counts
):
    dp = lax.axis_index(DP).astype(jnp.int32).reshape(1)
    scratch = [
        pltpu.VMEM(tokens.shape, BF16),
        pltpu.VMEM(cotangent.shape, BF16),
        pltpu.VMEM(slot_tokens.shape, jnp.int32),
        pltpu.VMEM(gate_weights.shape, F32),
        pltpu.SMEM((2,), jnp.int32),
        pltpu.SemaphoreType.DMA((5,)),
    ]
    (message,) = local(pick_kernel, [HB] * 5, [(MESSAGE, 128)], scratch=scratch)(
        *(
            in_hbm(a)
            for a in (tokens, cotangent, slot_tokens, gate_weights, live_counts.reshape(2))
        )
    )
    swap = [(0, 1), (1, 0)]
    message = lax.ppermute(message, EVERY, outward())
    far = [lax.ppermute(w, "c", swap) for w in (gate_proj, up_proj, down_proj)]
    held = [in_vmem(w) for w in (gate_proj, far[0], up_proj)]
    copies = jnp.broadcast_to(message[None], (ZL, MESSAGE, 128))
    column = lax.all_to_all(copies, "zl", 0, 0, tiled=True)
    got = in_vmem(lax.all_gather(column, "y", axis=0, tiled=False))

    parts, far_up = local(
        forward_kernel,
        [SM] + [VM] * 4 + [HB] * 3,
        [(X, 6, ZH * R, 512), up_proj.shape],
        scratch=[pltpu.VMEM(down_proj.shape, BF16)] * 2 + [pltpu.SemaphoreType.DMA((3,))],
    )(dp, got, *held, *(in_hbm(w) for w in (far[1], down_proj, far[2])))
    (loan,) = local(loan_kernel, [SM, VM], [(2, ZL, MESSAGE, 128)])(dp, got)
    lent = lax.ppermute(loan, "c", swap)
    over_x = lax.all_to_all(parts, "x", 0, 0, tiled=True)
    over_x = folded(over_x)
    over_zh = lax.all_gather(over_x, "zh", axis=0, tiled=False)
    sums = jnp.sum(over_zh.astype(F32), axis=0)
    gate_sum, up_sum, cot_hidden = sums[0:2], sums[2:4], sums[4:6]
    sigmoid_part = jax.nn.sigmoid(gate_sum)
    hidden = gate_sum * sigmoid_part * up_sum
    grad_gate = cot_hidden * up_sum * sigmoid_part * (1.0 + gate_sum * (1.0 - sigmoid_part))
    grad_up = cot_hidden * gate_sum * sigmoid_part
    acts = jnp.concatenate([hidden, grad_gate, grad_up], axis=0).astype(BF16)
    mine = lax.all_gather(acts, "x", axis=0, tiled=False)
    other = lax.ppermute(mine, "c", swap)
    mine = in_vmem(mine)

    (back,) = local(back_kernel, [SM] + [VM] * 5, [(Y, ZL, PACK, 128)])(dp, mine, *held, far_up)
    over_y = lax.all_to_all(back, "y", 0, 0, tiled=True)
    over_y = folded(over_y, False)
    over_zl = lax.all_to_all(over_y, "zl", 0, 0, tiled=True)
    over_zl = jnp.sum(over_zl.astype(F32), axis=0).astype(BF16)
    home = lax.ppermute(over_zl, EVERY, homeward())
    home = in_vmem(home)
    grad_gate_proj, grad_up_proj, grad_down_proj = local(
        weight_kernel,
        [SM, VM, VM, VM, VM],
        [gate_proj.shape, up_proj.shape, down_proj.shape],
        False,
    )(dp, got, lent, mine, other)
    (grad_tokens,) = local(place_kernel, [VM, VM], [tokens.shape], False)(home, slot_tokens)
    return (grad_tokens, grad_gate_proj, grad_up_proj, grad_down_proj)


def solution(mesh):
    fine = Mesh(mesh.devices.reshape(X, ZH, C, ZL, Y), EVERY)
    in_specs = (
        P(DP, SHARD),
        P(DP, SHARD),
        P(None, DP, SHARD),
        P(None, DP, SHARD),
        P(None, SHARD, DP),
        P(None, DP),
        P(None, DP),
        P(None, DP),
    )
    out_specs = (
        P(DP, SHARD),
        P(None, DP, SHARD),
        P(None, DP, SHARD),
        P(None, SHARD, DP),
    )
    return jax.shard_map(layer, mesh=fine, in_specs=in_specs, out_specs=out_specs, check_vma=False)
```

```python
import jax
import jax.numpy as jnp
from jax import lax
from jax.experimental import pallas as pl
from jax.experimental.pallas import tpu as pltpu
from jax.sharding import Mesh, PartitionSpec as P

X, ZH, C, ZL, Y = 4, 2, 2, 8, 4
DP = ("x", "zh", "c")
SHARD = ("zl", "y")
EVERY = DP + SHARD
N_SHARD = ZL * Y
HALF = 192
R = 16
PACK = 3 * R
MESSAGE = 2 * PACK + 8
BF16 = jnp.bfloat16
F32 = jnp.float32


def ring(a, b, n):
    return min((a - b) % n, (b - a) % n)


def columns(zl):
    x_here, zh_here = divmod(zl, ZH)
    by_reach = sorted(range(ZL), key=lambda p: (abs(p - zl), p))
    by_ring = sorted(range(X), key=lambda x: (-ring(x, x_here, X), x))
    near = {(x, zh_here): p for x, p in zip(by_ring, by_reach[:4])}
    far = {(x, 1 - zh_here): p for x, p in zip(by_ring, by_reach[:3:-1])}
    return near | far


def outward():
    pairs = []
    for k in range(X * ZH * C):
        x, zh, c = k // 4, k // 2 % 2, k % 2
        for s in range(N_SHARD):
            zl, y = divmod(s, Y)
            there = zl * C + c
            column = columns(zl)[(x, zh)]
            pairs.append((k * N_SHARD + s, there * N_SHARD + column * Y + y))
    return pairs


def code_of(zl):
    return sum(p << 3 * (ZH * x + zh) for (x, zh), p in columns(zl).items())


class Slots:
    def __init__(self, dp_ref):
        self.core = dp_ref[0] & 1
        zl = dp_ref[0] >> 1
        self.code = sum(jnp.where(zl == i, code_of(i), 0) for i in range(ZL))

    def halves(self):
        return (self.core, 1 - self.core)

    def column(self, j):
        return (self.code >> 3 * j) & 7


def homeward():
    return [(there, here) for here, there in outward()]


def dot(a, b, dims):
    return lax.dot_general(a, b, (dims, ((), ())), preferred_element_type=F32)


def as_column(row):
    n = row.shape[1]
    eye = lax.broadcasted_iota(jnp.int32, (n, n), 0) == lax.broadcasted_iota(jnp.int32, (n, n), 1)
    return jnp.sum(jnp.where(eye, jnp.broadcast_to(row, (n, n)), 0), axis=1, keepdims=True)


def pick_kernel(
    tok_hbm, cot_hbm, slot_hbm, gate_hbm, live_hbm, out_ref, tok, cot, slots, gates, live, sems
):
    moves = [
        pltpu.make_async_copy(source, target, sems.at[i])
        for i, (source, target) in enumerate(
            (
                (slot_hbm, slots),
                (gate_hbm, gates),
                (live_hbm, live),
                (tok_hbm, tok),
                (cot_hbm, cot),
            )
        )
    ]
    for move in moves:
        move.start()
    for move in moves:
        move.wait()
    spot = lax.broadcasted_iota(jnp.int32, (R, 64), 1)
    row = lax.broadcasted_iota(jnp.int32, (R, 1), 0)
    one_hot = [(as_column(slots[e : e + 1, :]) == spot).astype(BF16) for e in range(2)]
    scale = [jnp.where(row < live[e], as_column(gates[e : e + 1, :]), 0.0) for e in range(2)]
    for m, in_ref in enumerate((tok, cot)):
        values = in_ref[...]
        rows = [dot(one_hot[e], values, ((1,), (0,))) for e in range(2)]
        if m == 1:
            rows = [rows[e] * scale[e] for e in range(2)]
        out_ref[m * PACK : (m + 1) * PACK, :] = packed([part.astype(BF16) for part in rows])
    lane = lax.broadcasted_iota(jnp.int32, (8, 128), 1)
    line = lax.broadcasted_iota(jnp.int32, (8, 128), 0)
    note = jnp.where(lane == 0, live[0], 0) + jnp.where(lane == 64, live[1], 0)
    out_ref[2 * PACK :, :] = jnp.where(line == 0, note, 0).astype(F32).astype(BF16)


def packed(rows):
    left = jnp.concatenate([part[:, 128:] for part in rows], axis=1)
    return jnp.concatenate([part[:, :128] for part in rows] + [left], axis=0)


def features(at, slots, m, e):
    blocks = []
    for j in range(ZH * X):
        parts = []
        for h in range(2):
            block = at(h, slots.column(j))
            parts.append(block[m * PACK + e * R : m * PACK + (e + 1) * R, :])
            left = block[m * PACK + 2 * R : (m + 1) * PACK, :]
            parts.append(left[:, e * 64 : (e + 1) * 64])
        blocks.append(jnp.concatenate(parts, axis=1))
    return jnp.concatenate(blocks, axis=0)


def lines_of(got_ref, half):
    return lambda h, column: got_ref.at[2 * half + h, column]


def forward_kernel(
    dp_ref, got_ref, gate_ref, far_gate, up_ref, up_hbm, down_hbm, far_hbm, out_ref, far_up, *scratch
):
    down_ref, far_down, sems = scratch
    moves = [
        pltpu.make_async_copy(source, target, sems.at[i])
        for i, (source, target) in enumerate(
            ((down_hbm, down_ref), (up_hbm, far_up), (far_hbm, far_down))
        )
    ]
    for move in moves:
        move.start()
    slots = Slots(dp_ref)

    def finish(t, e, part):
        out_ref[:, 2 * t + e] = part.astype(BF16).reshape(X, ZH * R, 512)

    def give(t, e, rows, pair, dims):
        finish(t, e, dot(rows[0], pair[0][e], dims) + dot(rows[1], pair[1][e], dims))

    def both(m, e):
        return [features(lines_of(got_ref, half), slots, m, e) for half in slots.halves()]

    rows = [both(0, e) for e in range(2)]
    cots = [both(1, e) for e in range(2)]
    inward, across = ((1,), (0,)), ((1,), (1,))
    for e in range(2):
        give(0, e, rows[e], (gate_ref, far_gate), inward)
    near_up = [dot(rows[e][0], up_ref[e], inward) for e in range(2)]
    moves[0].wait()
    near_cot = [dot(cots[e][0], down_ref[e], across) for e in range(2)]
    moves[1].wait()
    for e in range(2):
        finish(1, e, near_up[e] + dot(rows[e][1], far_up[e], inward))
    moves[2].wait()
    for e in range(2):
        finish(2, e, near_cot[e] + dot(cots[e][1], far_down[e], across))


def loan_kernel(dp_ref, got_ref, out_ref):
    slots = Slots(dp_ref)
    for h in range(2):
        out_ref[h] = got_ref[2 * (1 - slots.core) + h]


def fold_kernel(in_ref, out_ref):
    total = sum(in_ref[i].astype(F32) for i in range(in_ref.shape[0]))
    out_ref[...] = total.astype(BF16)


def all_rows(refs, t, e):
    return jnp.concatenate([ref[:, 2 * t + e].reshape(ZH * X * R, 512) for ref in refs], axis=0)


def back_kernel(dp_ref, mine_ref, gate_ref, far_gate, up_ref, far_up, out_ref):
    slots = Slots(dp_ref)
    grads = [[all_rows((mine_ref,), t, e) for t in (1, 2)] for e in range(2)]
    for half, weights in zip(slots.halves(), ((gate_ref, up_ref), (far_gate, far_up))):
        terms = [
            sum(dot(grads[e][t], weights[t][e], ((1,), (1,))) for t in range(2)).astype(BF16)
            for e in range(2)
        ]
        for h in range(2):
            for j in range(ZH * X):
                rows = [term[j * R : (j + 1) * R, h * HALF : (h + 1) * HALF] for term in terms]
                out_ref[2 * half + h, slots.column(j)] = packed(rows)


def weight_kernel(dp_ref, got_ref, lent_ref, mine_ref, other_ref, gate_out, up_out, down_out):
    slots = Slots(dp_ref)
    notes = [ref[0, :, 2 * PACK :, :].astype(F32).reshape(ZL * 8, 128) for ref in (got_ref, lent_ref)]
    notes = jnp.concatenate(notes, axis=0)
    acts = (mine_ref, other_ref)
    for e in range(2):
        scale = 1.0 / jnp.full((1, 512), jnp.sum(notes[:, e * 64 : (e + 1) * 64]), F32)
        rows, cot = (
            jnp.concatenate(
                [
                    features(lines_of(got_ref, slots.core), slots, m, e),
                    features(lines_of(lent_ref, 0), slots, m, e),
                ],
                axis=0,
            )
            for m in range(2)
        )
        hidden, grad_gate, grad_up = (all_rows(acts, t, e) for t in range(3))
        gate_out[e] = (dot(rows, grad_gate, ((0,), (0,))) * scale).astype(BF16)
        up_out[e] = (dot(rows, grad_up, ((0,), (0,))) * scale).astype(BF16)
        down_out[e] = (dot(hidden, cot, ((0,), (0,))) * scale[:, :384]).astype(BF16)


def place_kernel(rows_ref, slot_ref, out_ref):
    spot = lax.broadcasted_iota(jnp.int32, (64, R), 0)
    total = jnp.zeros((64, HALF), F32)
    left = rows_ref[2 * R :, :]
    for e in range(2):
        one_hot = (spot == slot_ref[e : e + 1, :]).astype(BF16)
        rows = [rows_ref[e * R : (e + 1) * R, :], left[:, e * 64 : (e + 1) * 64]]
        total = total + dot(one_hot, jnp.concatenate(rows, axis=1), ((1,), (0,)))
    out_ref[...] = total.astype(BF16)


VM = pl.BlockSpec(memory_space=pltpu.VMEM)
SM = pl.BlockSpec(memory_space=pltpu.SMEM)
HB = pl.BlockSpec(memory_space=pltpu.HBM)


def in_vmem(x):
    return pltpu.with_memory_space_constraint(x, pltpu.VMEM)


def in_hbm(x):
    return pltpu.with_memory_space_constraint(x, pltpu.HBM)


def local(kernel, specs, outs, stay=True, scratch=()):
    if stay:
        shapes = [pltpu.VMEM(o, BF16) for o in outs]
    else:
        shapes = [pltpu.HBM(o, BF16) for o in outs]
    return pl.pallas_call(
        kernel,
        in_specs=specs,
        out_specs=[VM] * len(outs),
        out_shape=shapes,
        scratch_shapes=scratch,
        compiler_params=pltpu.CompilerParams(vmem_limit_bytes=16 << 20),
    )


def folded(tiles, stay=True):
    (total,) = local(fold_kernel, [VM], [tiles.shape[1:]], stay)(in_vmem(tiles))
    return total


def layer(
    tokens, cotangent, gate_proj, up_proj, down_proj, slot_tokens, gate_weights, live_counts
):
    dp = lax.axis_index(DP).astype(jnp.int32).reshape(1)
    scratch = [
        pltpu.VMEM(tokens.shape, BF16),
        pltpu.VMEM(cotangent.shape, BF16),
        pltpu.VMEM(slot_tokens.shape, jnp.int32),
        pltpu.VMEM(gate_weights.shape, F32),
        pltpu.SMEM((2,), jnp.int32),
        pltpu.SemaphoreType.DMA((5,)),
    ]
    (message,) = local(pick_kernel, [HB] * 5, [(MESSAGE, 128)], scratch=scratch)(
        *(
            in_hbm(a)
            for a in (tokens, cotangent, slot_tokens, gate_weights, live_counts.reshape(2))
        )
    )
    swap = [(0, 1), (1, 0)]
    message = lax.ppermute(message, EVERY, outward())
    far = [lax.ppermute(w, "c", swap) for w in (gate_proj, up_proj, down_proj)]
    held = [in_vmem(w) for w in (gate_proj, far[0], up_proj)]
    copies = jnp.broadcast_to(message[None], (ZL, MESSAGE, 128))
    column = lax.all_to_all(copies, "zl", 0, 0, tiled=True)
    got = in_vmem(lax.all_gather(column, "y", axis=0, tiled=False))

    parts, far_up = local(
        forward_kernel,
        [SM] + [VM] * 4 + [HB] * 3,
        [(X, 6, ZH * R, 512), up_proj.shape],
        scratch=[pltpu.VMEM(down_proj.shape, BF16)] * 2 + [pltpu.SemaphoreType.DMA((3,))],
    )(dp, got, *held, *(in_hbm(w) for w in (far[1], down_proj, far[2])))
    (loan,) = local(loan_kernel, [SM, VM], [(2, ZL, MESSAGE, 128)])(dp, got)
    lent = lax.ppermute(loan, "c", swap)
    over_x = lax.all_to_all(parts, "x", 0, 0, tiled=True)
    over_x = folded(over_x)
    over_zh = lax.all_gather(over_x, "zh", axis=0, tiled=False)
    sums = jnp.sum(over_zh.astype(F32), axis=0)
    gate_sum, up_sum, cot_hidden = sums[0:2], sums[2:4], sums[4:6]
    sigmoid_part = jax.nn.sigmoid(gate_sum)
    hidden = gate_sum * sigmoid_part * up_sum
    grad_gate = cot_hidden * up_sum * sigmoid_part * (1.0 + gate_sum * (1.0 - sigmoid_part))
    grad_up = cot_hidden * gate_sum * sigmoid_part
    acts = jnp.concatenate([hidden, grad_gate, grad_up], axis=0).astype(BF16)
    mine = lax.all_gather(acts, "x", axis=0, tiled=False)
    other = lax.ppermute(mine, "c", swap)
    mine = in_vmem(mine)

    (back,) = local(back_kernel, [SM] + [VM] * 5, [(Y, ZL, PACK, 128)])(dp, mine, *held, far_up)
    over_y = lax.all_to_all(back, "y", 0, 0, tiled=True)
    over_y = folded(over_y, False)
    over_zl = lax.all_to_all(over_y, "zl", 0, 0, tiled=True)
    over_zl = jnp.sum(over_zl.astype(F32), axis=0).astype(BF16)
    home = lax.ppermute(over_zl, EVERY, homeward())
    home = in_vmem(home)
    grad_gate_proj, grad_up_proj, grad_down_proj = local(
        weight_kernel,
        [SM, VM, VM, VM, VM],
        [gate_proj.shape, up_proj.shape, down_proj.shape],
        False,
    )(dp, got, lent, mine, other)
    (grad_tokens,) = local(place_kernel, [VM, VM], [tokens.shape], False)(home, slot_tokens)
    return (grad_tokens, grad_gate_proj, grad_up_proj, grad_down_proj)


def solution(mesh):
    fine = Mesh(mesh.devices.reshape(X, ZH, C, ZL, Y), EVERY)
    in_specs = (
        P(DP, SHARD),
        P(DP, SHARD),
        P(None, DP, SHARD),
        P(None, DP, SHARD),
        P(None, SHARD, DP),
        P(None, DP),
        P(None, DP),
        P(None, DP),
    )
    out_specs = (
        P(DP, SHARD),
        P(None, DP, SHARD),
        P(None, DP, SHARD),
        P(None, SHARD, DP),
    )
    return jax.shard_map(layer, mesh=fine, in_specs=in_specs, out_specs=out_specs, check_vma=False)
```
